32 devices in a mesh: gx: 2 (over x), gy: 4 (over z), gz: 4 (over y, core).
Axes of the slice: x: 2, y: 2, z: 4, core: 2. Of those that a mesh axis runs over, the one named last changes fastest.
Arguments:
- displacement: bfloat16 [3, 8, 128, 64], P(None, 'gx', 'gy', 'gz'), may hold values from -6 to 6
- lift_weight: bfloat16 [27, 64, 3], replicated, may hold values from -1 to 1
- encode_weight: bfloat16 [27, 64, 64], replicated, may hold values from -0.21875 to 0.21875
- downward_weight: bfloat16 [8, 128, 64], replicated, may hold values from -0.375 to 0.375
- middle_first: bfloat16 [27, 128, 128], replicated, may hold values from -0.15625 to 0.15625
- middle_second: bfloat16 [27, 128, 128], replicated, may hold values from -0.15625 to 0.15625
- up_weight: bfloat16 [8, 64, 128], replicated, may hold values from -0.75 to 0.75
- decode_weight: bfloat16 [27, 64, 128], replicated, may hold values from -0.15625 to 0.15625
- head_weight: bfloat16 [3, 64], replicated, may hold values from -1 to 1
Outputs:
- imitated: float32 [3, 8, 128, 64], P(None, 'gx', 'gy', 'gz')
The draws below stay inside these ranges and needn't reach their ends.
All inputs are finite; a program needn't handle non-finite values.
Results may differ from the reference program's by a relative error of at most 0.0055.
Values may be sent and summed in bfloat16 or wider, within the bound.
A program may use at most 64 MiB of HBM per device.

```python
import jax
import jax.numpy as jnp

C1 = 64
C2 = 128
NX = 8
NY = 128
NZ = 64


def levels(stream_key, shape, pieces, low, top_value):
    loudness, own = 1.0, jax.random.fold_in(stream_key, 6)
    for position, parts in pieces:
        steps = jnp.exp(jax.random.uniform(jax.random.fold_in(own, position), (parts,), jnp.float32, low / len(pieces), top_value / len(pieces)))
        loudness = loudness * jnp.repeat(steps, shape[position] // parts).reshape([-1 if axis == position else 1 for axis in range(len(shape))])
    return loudness


def noise(stream_key, shape, scale, bound, shards=(), kind=jnp.bfloat16):
    entries = jax.random.normal(stream_key, shape, jnp.float32) * scale
    if len(shards) > 0:
        entries = levels(stream_key, shape, shards, -0.22, 0.18) * entries
    return jnp.clip(entries, min=-bound, max=bound).astype(kind)


def setup_inputs(seed: int = 0) -> dict:
    streams_of = jax.random.split(jax.random.key(seed), 10)
    return {
        "displacement": noise(streams_of[0], (3, NX, NY, NZ), 1.0, 6.0, ((1, 2), (2, 4), (3, 4))),
        "lift_weight": noise(streams_of[1], (27, C1, 3), (81 // 2) ** -0.5, 1.0),
        "encode_weight": noise(streams_of[2], (27, C1, C1), (27 * C1 // 2) ** -0.5, 0.21875),
        "downward_weight": noise(streams_of[3], (8, C2, C1), (4 * C1) ** -0.5, 0.375),
        "middle_first": noise(streams_of[4], (27, C2, C2), (27 * C2 // 2) ** -0.5, 0.15625),
        "middle_second": noise(streams_of[5], (27, C2, C2), (27 * C2 // 2) ** -0.5, 0.15625),
        "up_weight": noise(streams_of[6], (8, C1, C2), (C2 // 2) ** -0.5, 0.75),
        "decode_weight": noise(streams_of[7], (27, C1, 2 * C1), (27 * C1) ** -0.5, 0.15625),
        "head_weight": noise(streams_of[8], (3, C1), (C1 // 2) ** -0.5, 1.0),
    }


def apply_relu(value):
    return jnp.where(value > 0, value, 0.1 * value)


def conv_periodic(field, weight_tensor):
    padded = jnp.pad(field, ((0, 0), (1, 1), (1, 1), (1, 1)), mode="wrap")
    size_x, size_y, size_z = field.shape[1], field.shape[2], field.shape[3]
    weights32 = weight_tensor.astype(jnp.float32)
    summed = jnp.zeros((weight_tensor.shape[1], size_x, size_y, size_z), jnp.float32)
    for offset in range(27):
        a, b, c = offset // 9, (offset // 3) % 3, offset % 3
        window = padded[:, a:a + size_x, b:b + size_y, c:c + size_z].astype(jnp.float32)
        summed = summed + jnp.einsum("oi,ixyz->oxyz", weights32[offset], window)
    return summed


def reduce_resolution(fine_level, weight_tensor):
    chans, size_x, size_y, size_z = fine_level.shape
    blocks = fine_level.reshape(chans, size_x // 2, 2, size_y // 2, 2, size_z // 2, 2).astype(jnp.float32)
    kernel = weight_tensor.reshape(2, 2, 2, weight_tensor.shape[1], weight_tensor.shape[2]).astype(jnp.float32)
    return jnp.einsum("abcoi,ixaybzc->oxyz", kernel, blocks)


def upsample(coarse_field, weight_tensor):
    chans, size_x, size_y, size_z = coarse_field.shape
    kernel = weight_tensor.reshape(2, 2, 2, weight_tensor.shape[1], weight_tensor.shape[2]).astype(jnp.float32)
    result = jnp.einsum("abcoi,ixyz->oxaybzc", kernel, coarse_field.astype(jnp.float32))
    return result.reshape(weight_tensor.shape[1], 2 * size_x, 2 * size_y, 2 * size_z)


def reference(displacement, lift_weight, encode_weight, downward_weight, middle_first, middle_second, up_weight, decode_weight, head_weight):
    first = apply_relu(conv_periodic(displacement, lift_weight)).astype(jnp.bfloat16)
    skip_link = apply_relu(conv_periodic(first, encode_weight)).astype(jnp.bfloat16)
    coarse_level = apply_relu(reduce_resolution(skip_link, downward_weight)).astype(jnp.bfloat16)
    middle = apply_relu(conv_periodic(coarse_level, middle_first)).astype(jnp.bfloat16)
    deep = apply_relu(conv_periodic(middle, middle_second)).astype(jnp.bfloat16)
    upsampled = apply_relu(upsample(deep, up_weight)).astype(jnp.bfloat16)
    stacked = jnp.concatenate([skip_link, upsampled], axis=0)
    joined = apply_relu(conv_periodic(stacked, decode_weight)).astype(jnp.bfloat16)
    head = jnp.einsum("oi,ixyz->oxyz", head_weight.astype(jnp.float32), joined.astype(jnp.float32))
    return displacement.astype(jnp.float32) + head
```

```python
import functools

import jax
import jax.numpy as jnp
from jax import lax
from jax.experimental import pallas as pl
from jax.experimental.pallas import tpu as pltpu
from jax.sharding import PartitionSpec as P

MESH = pl.DeviceIdType.MESH
NT = (((1,), (1,)), ((), ()))
NN = (((1,), (0,)), ((), ()))
F32, BF16 = jnp.float32, jnp.bfloat16
TILE, LANES = 8, 128


def leaky(value):
    return jnp.maximum(value, 0.1 * value)


def rounded(value):
    return leaky(value).astype(BF16)


def dot(rows, weight):
    return lax.dot_general(rows, weight, NT, preferred_element_type=F32)


def build_fine(raw, wide, lo, hi):
    out = raw.shape[1]
    blank = jnp.zeros((2 * out, wide.shape[2]), BF16)
    zero = jnp.zeros((out, hi - lo), BF16)
    for a in range(3):
        wide[4 * a, 2 * out :, :] = blank
        wide[4 * a + 3, : 2 * out, :] = blank
        for b in range(3):
            taps = [raw[9 * a + 3 * b + c][:, lo:hi] for c in range(3)]
            low = jnp.concatenate([taps[1], taps[2], zero, taps[0]], axis=1)
            high = jnp.concatenate([taps[0], taps[1], taps[2], zero], axis=1)
            pair = jnp.concatenate([low, high], axis=0)
            wide[4 * a + b, : 2 * out, :] = pair
            wide[4 * a + b + 1, 2 * out :, :] = pair


def build_coarse(raw, wide):
    out = raw.shape[1]
    blank = jnp.zeros((out, raw.shape[2]), BF16)
    for a in range(3):
        for b in range(3):
            for offset in range(2):
                tile = 6 * a + 2 * b + offset
                for side in range(2):
                    for e in range(2):
                        c = 2 * offset + e - side
                        block = raw[9 * a + 3 * b + c] if 0 <= c <= 2 else blank
                        wide[tile, out * side : out * (side + 1), LANES * e : LANES * (e + 1)] = block


def unet(
    dims,
    cells_hbm, lift_hbm, encode_hbm, downward_hbm, first_hbm, second_hbm, up_hbm, decode_hbm,
    head_hbm,
    out_ref,
    cells, lift_raw, head_raw, pack, window, joint, near, spread, lift_f, lift_rows, lift_w, select_w, chunks,
    fine_in, skip_scr, skip_in, wide_in, coarse_in, middle_in, deep_scr, up_scr, mine, final,
    head_f, head_w,
    encode_raw, downward_w, first_raw, second_raw, up_w, decode_raw,
    encode_w, skip_w, wide_w, first_w, second_w,
    load_sems, send_sems, recv_sems, swap_sems,
):
    ring_x, ring_y, ring_z = dims
    comps, size_x, size_z, size_y = cells.shape
    around = ring_x == 2
    steps = (0,) if around else (-1, 0, 1)
    pairs = ring_x // 2
    gx, gy, gz = lax.axis_index("gx"), lax.axis_index("gy"), lax.axis_index("gz")
    mine_x, pair = lax.rem(gx, 2), lax.div(gx, 2)

    def device(step, flip, shift_y, shift_z):
        side = 1 - mine_x if flip else mine_x
        return (
            2 * lax.rem(pair + pairs + step, pairs) + side,
            lax.rem(gy + ring_y + shift_y, ring_y),
            lax.rem(gz + ring_z + shift_z, ring_z),
        )

    links = [
        (step, flip, beside, dz)
        for step in steps for flip in (0, 1) for beside in (0, 1) for dz in (-1, 0, 1)
        if (step, flip, beside, dz) != (0, 0, 0, 0)
    ]
    barrier = pltpu.get_barrier_semaphore()
    for step, flip, beside, dz in links:
        shift = 2 * mine_x - 1 if beside else 0
        pl.semaphore_signal(
            barrier, inc=1, device_id=device(step, flip, shift, -dz), device_id_type=MESH
        )
    loads = [
        pltpu.make_async_copy(src, dst, load_sems.at[i])
        for i, (src, dst) in enumerate(
            (
                (cells_hbm, cells), (lift_hbm, lift_raw), (encode_hbm, encode_raw),
                (downward_hbm, downward_w), (first_hbm, first_raw), (second_hbm, second_raw),
                (up_hbm, up_w), (decode_hbm, decode_raw), (head_hbm, head_raw),
            )
        )
    ]
    for load in loads:
        load.start()

    loads[0].wait()
    for c in range(comps):
        total = None
        for x in range(size_x):
            value = cells[c, x].astype(F32)
            value = jnp.concatenate(
                [value, jnp.zeros((size_z, LANES - size_y), F32)], axis=1
            )
            value = pltpu.roll(value, size_y * x, 1) if x else value
            total = value if total is None else total + value
        pack[c] = total.reshape(size_z // TILE, TILE, LANES).astype(BF16)
    own_slot = mine_x if around else mine_x + 2
    tiles = size_z // TILE
    window[own_slot, 1 - mine_x, :, pl.ds(1, tiles)] = pack[...]
    pl.semaphore_wait(barrier, len(links))
    copies = []
    for number, (step, flip, beside, dz) in enumerate(links):
        side = 1 - mine_x if flip else mine_x
        shift = 1 - 2 * side if beside else 0
        row_slot = side if beside else 1 - side
        slot = mine_x if around else mine_x + 2 * (step + 1)
        start, count, place = {0: (0, tiles, 1), 1: (tiles - 1, 1, 0), -1: (0, 1, tiles + 1)}[dz]
        copies.append(
            pltpu.make_async_remote_copy(
                src_ref=pack.at[:, pl.ds(start, count)],
                dst_ref=window.at[slot, row_slot, :, pl.ds(place, count)],
                send_sem=send_sems.at[number], recv_sem=recv_sems.at[number],
                device_id=device(-step, flip, shift, dz), device_id_type=MESH,
            )
        )
    for copy in copies:
        copy.start()

    loads[1].wait()
    quarters = (size_z + 2 * TILE) // TILE
    slot_lanes = LANES // quarters
    for c in range(comps):
        value = lift_raw[c].astype(F32)
        spread[c] = jnp.concatenate([value, value], axis=1)
    depth = lift_w.shape[0]
    lift_f[pl.ds(0, depth), :] = jnp.zeros((depth, LANES), F32)
    for t in range(9):
        for cz in range(3):
            for c in range(comps):
                lift_f[pl.ds(slot_lanes * t + comps * cz + c, 1), :] = spread[
                    c, pl.ds(3 * t + cz, 1), :
                ]
    base = lift_f[pl.ds(0, depth), :]
    low_half = lax.broadcasted_iota(jnp.int32, (depth, LANES), 1) < LANES // 2
    for k in range(TILE // 2):
        even = pltpu.roll(base, comps * 2 * k, 0) if k else base
        odd = pltpu.roll(base, comps * (2 * k + 1), 0)
        lift_w[:, LANES * k : LANES * (k + 1)] = jnp.where(low_half, even, odd).astype(BF16)

    rows_s, lanes_s = select_w.shape
    zw = size_z + 2 * TILE
    row = lax.broadcasted_iota(jnp.int32, (rows_s, LANES), 0)
    lane = lax.broadcasted_iota(jnp.int32, (rows_s, LANES), 1)
    place, inside = lax.div(lane, slot_lanes), lax.rem(lane, slot_lanes)
    level = lax.div(inside, comps)
    comp = inside - comps * level
    for k in range(quarters):
        source = lax.rem(place + quarters - k, quarters)
        target = comp * zw + TILE * source - 1 + level
        hit = (row == target) & (inside < comps * (TILE + 2))
        select_w[:, LANES * k : LANES * (k + 1)] = jnp.where(hit, 1.0, 0.0).astype(BF16)

    loads[2].wait()
    build_fine(encode_raw, encode_w, 0, encode_raw.shape[2])
    loads[4].wait()
    build_coarse(first_raw, first_w)
    loads[5].wait()
    build_coarse(second_raw, second_w)
    loads[7].wait()
    channels = decode_raw.shape[2] // 2
    build_fine(decode_raw, skip_w, 0, channels)
    build_fine(decode_raw, wide_w, channels, 2 * channels)
    loads[8].wait()
    head_f[...] = jnp.zeros(head_f.shape, F32)
    for p in range(2):
        for q in range(2):
            for c in range(comps):
                value = head_raw[pl.ds(c, 1), :].astype(F32)
                other = jnp.zeros_like(value)
                head_f[
                    pl.ds(LANES * p + size_z * c + q, 1), LANES * p : LANES * (p + 1)
                ] = jnp.concatenate([other, value] if q else [value, other], axis=1)
    head_w[...] = head_f[...].astype(BF16)
    loads[3].wait()
    loads[6].wait()

    for copy in copies:
        copy.wait_recv()

    slots = window.shape[0]
    turned = jnp.concatenate(
        [
            jnp.swapaxes(window[s, r].astype(F32).reshape(comps * zw, LANES), 0, 1)
            for s in range(slots) for r in range(2)
        ],
        axis=0,
    ).astype(BF16)
    grouped = lax.dot_general(turned, select_w[...], NN, preferred_element_type=F32)
    tiles_y = size_y // TILE
    for s in range(slots):
        for r in range(2):
            part = grouped[LANES * (2 * s + r) : LANES * (2 * s + r + 1)]
            for k in range(quarters):
                joint[k, pl.ds(size_x * s, size_x), pl.ds(tiles_y * r, tiles_y)] = part[
                    :, LANES * k : LANES * (k + 1)
                ].reshape(size_x, tiles_y, TILE, LANES)
    planes_d, rows_n = near.shape[1], near.shape[2]
    first_tile = tiles_y - 2 - (tiles_y // 2) * mine_x
    for k in range(quarters):
        for x in range(planes_d):
            near[k, x] = joint[k, x, pl.ds(first_tile, rows_n // TILE)].reshape(rows_n, LANES)

    planes_f, planes_s = fine_in.shape[1], skip_in.shape[1]
    planes_c, planes_m, planes_e = coarse_in.shape[1], middle_in.shape[1], deep_scr.shape[0]
    planes_u = wide_in.shape[1]

    def source(plane, tap, total, shift=0):
        if around:
            return lax.rem(plane + tap + total - 1, total)
        return plane + tap + shift

    half_y = rows_n // 3
    slot_of = lax.div(lax.broadcasted_iota(jnp.int32, (half_y, LANES), 1), slot_lanes)

    @pl.loop(0, planes_f)
    def _(x):
        for parity in range(2):
            for q in range(quarters):
                for g in range(3):
                    taps = list(range(quarters * g, min(quarters * (g + 1), 9)))
                    value = None
                    for j, t in enumerate(taps):
                        part = near[
                            (j - q) % quarters, source(x, t // 3, planes_d),
                            pl.ds(TILE - 1 + parity + t % 3, half_y, stride=2), :,
                        ]
                        value = part if value is None else jnp.where(slot_of < j, value, part)
                    lift_rows[
                        q, pl.ds(pl.multiple_of(2 * half_y * x + half_y * parity, half_y), half_y),
                        LANES * g : LANES * (g + 1),
                    ] = value.astype(BF16)

    for q in range(quarters):
        value = leaky(
            lax.dot_general(lift_rows[q], lift_w[...], NN, preferred_element_type=F32)
        ).astype(BF16).astype(F32)
        for r in range(quarters):
            chunks[quarters * q + r] = value[:, LANES * r : LANES * (r + 1)]

    zpairs = zw // 2
    half = lax.broadcasted_iota(jnp.int32, (2 * half_y, LANES), 1) < LANES // 2

    @pl.loop(0, planes_f)
    def _(x):
        span = pl.ds(pl.multiple_of(2 * half_y * x, 2 * half_y), 2 * half_y)
        for zp in range(1, zpairs - 1):
            plane = chunks[zp, span, :]
            twin = jnp.where(half, chunks[zp + 1, span, :], chunks[zp - 1, span, :])
            for number, value in enumerate((plane, twin)):
                even, odd = value[:half_y], value[half_y:]
                for b, part in enumerate(
                    (pltpu.roll(odd, 1, 0), even, odd, pltpu.roll(even, half_y - 1, 0))
                ):
                    fine_in[
                        b, x, half_y * (zp - 1) : half_y * zp,
                        LANES * number : LANES * (number + 1),
                    ] = part.astype(BF16)

    inner = zpairs - 2
    quarter = TILE // 2
    own = zpairs - TILE
    wide_half = lax.broadcasted_iota(jnp.int32, (own, TILE, LANES), 2) < LANES // 2

    def store_pairs(target, x, scr, first):
        for b in range(4):
            lanes = slice(LANES * ((b + 1) % 2), LANES * ((b + 1) % 2) + LANES)
            rows = pl.ds(quarter + (b - 1) // 2 if b % 2 == 0 else quarter + b // 2, TILE)
            plane, above, below = (
                scr[pl.ds(first + d, own), rows, lanes] for d in (0, 1, -1)
            )
            twin = jnp.where(wide_half, above, below)
            target[b, x] = jnp.concatenate(
                [plane.reshape(own * TILE, LANES), twin.reshape(own * TILE, LANES)], axis=1
            ).astype(BF16)

    def store_coarse(target, x, z, value):
        lanes = slice(LANES * (z % 2), LANES * (z % 2) + LANES)
        for b, part in enumerate((pltpu.roll(value, 1, 0), value, pltpu.roll(value, half_y - 1, 0))):
            target[b, x, z // 2, :, lanes] = part.astype(BF16)

    rows_e = inner * half_y

    @pl.loop(0, planes_c)
    def _(x):
        summed = None
        for a in range(3):
            for b in range(4):
                lhs = jnp.concatenate(
                    [fine_in[b, source(2 * x + g, a, planes_f)] for g in range(2)], axis=0
                )
                term = dot(lhs, encode_w[4 * a + b])
                summed = term if summed is None else summed + term
        skip = rounded(summed)
        coarse = None
        for g in range(2):
            part = skip[g * rows_e : (g + 1) * rows_e]
            term = lax.dot_general(part, downward_w[g], NN, preferred_element_type=F32)
            coarse = term if coarse is None else coarse + term
            skip_scr[g] = part.astype(F32).reshape(inner, half_y, 2 * LANES)
        coarse = rounded(coarse).astype(F32)
        for z in range(inner):
            store_coarse(coarse_in, x, z, coarse[half_y * z : half_y * (z + 1)])
        for g in range(2):
            store_pairs(skip_in, 2 * x + g, skip_scr.at[g], (inner - own) // 2)

    def coarse_conv(target, weight, planes, count):
        total = target.shape[1]
        summed = None
        for a in range(3):
            for b in range(3):
                for offset in range(2):
                    lhs = jnp.concatenate(
                        [
                            target[
                                b, (x + a - 1) % total if around else x + a,
                                offset : offset + count,
                            ].reshape(count * half_y, 2 * LANES)
                            for x in range(planes)
                        ],
                        axis=0,
                    )
                    term = dot(lhs, weight[6 * a + 2 * b + offset])
                    summed = term if summed is None else summed + term
        return rounded(summed)

    count = inner // 2 - 1
    middle = coarse_conv(coarse_in, first_w, planes_m, count).astype(F32)
    for x in range(planes_m):
        for z in range(2 * count):
            start = half_y * (count * x + z // 2)
            store_coarse(
                middle_in, x, z,
                middle[start : start + half_y, LANES * (z % 2) : LANES * (z % 2) + LANES],
            )
    count -= 1
    deep = coarse_conv(middle_in, second_w, planes_e, count)
    deep_scr[...] = deep.reshape(planes_e, count * half_y, 2 * LANES)

    @pl.loop(0, planes_e)
    def _(x):
        for a in range(2):
            for side in range(2):
                lhs = deep_scr[x, :, LANES * side : LANES * (side + 1)]
                value = rounded(dot(lhs, up_w[a])).astype(F32)
                for u in range(count):
                    up_scr[a, 2 * u + side] = value[half_y * u : half_y * (u + 1)]
        for a in range(2):
            store_pairs(wide_in, 2 * x + a, up_scr.at[a], count - own // 2)

    swap = None
    for turn in range(2):
        side = mine_x if turn else 1 - mine_x
        summed = None
        for array, weight, shift in ((skip_in, skip_w, 5), (wide_in, wide_w, 1)):
            total = array.shape[1]
            for a in range(3):
                for b in range(4):
                    lhs = jnp.concatenate(
                        [
                            array[b, source(size_x * side + g, a, total, shift)]
                            for g in range(size_x)
                        ],
                        axis=0,
                    )
                    term = dot(lhs, weight[4 * a + b])
                    summed = term if summed is None else summed + term
        result = dot(rounded(summed), head_w[...])
        for g in range(size_x):
            for p in range(2):
                total = None
                for z in range(own):
                    start = TILE * (own * g + z)
                    value = result[start : start + TILE, LANES * p : LANES * (p + 1)]
                    value = pltpu.roll(value, 2 * z, 1) if z else value
                    total = value if total is None else total + value
                if turn:
                    final[g, mine_x, pl.ds(p, TILE, stride=2), :] = total
                else:
                    mine[g, pl.ds(p, TILE, stride=2), :] = total
        if not turn:
            swap = pltpu.make_async_remote_copy(
                src_ref=mine, dst_ref=final.at[:, mine_x],
                send_sem=swap_sems.at[0], recv_sem=swap_sems.at[1],
                device_id=device(0, 1, 0, 0), device_id_type=MESH,
            )
            swap.start()
    swap.wait_recv()
    flat = jnp.swapaxes(final[...].reshape(LANES, LANES), 0, 1)
    for c in range(comps):
        block = flat[size_z * c : size_z * (c + 1)]
        for x in range(size_x):
            value = pltpu.roll(block, LANES - size_y * x, 1) if x else block
            out_ref[c, x] = cells[c, x].astype(F32) + value[:, :size_y]
    for copy in copies:
        copy.wait_send()
    swap.wait_send()


def local(
    rings, displacement, lift_weight, encode_weight, downward_weight, middle_first, middle_second,
    up_weight, decode_weight, head_weight,
):
    comps, size_x, size_y, size_z = displacement.shape
    c1, c2 = encode_weight.shape[1], middle_first.shape[1]
    around = rings[0] == 2
    slots = 2 if around else 6
    span = 2 * size_x
    halo = (lambda h: 0) if around else (lambda h: h)
    zw, yh = size_z + 2 * TILE, (size_y // 2 + 2 * TILE) // 2
    zpairs, quarters = zw // 2, zw // TILE
    planes_d, planes_f, planes_s = (span + 2 * halo(h) for h in (8, 7, 6))
    planes_c, planes_m, planes_e = (span // 2 + 2 * halo(h) for h in (3, 2, 1))
    depth = 3 * LANES

    cells = jnp.transpose(displacement, (0, 1, 3, 2))
    lift = jnp.transpose(lift_weight, (2, 0, 1))
    downward = jnp.transpose(downward_weight, (0, 2, 1)).reshape(2, 4 * c1, c2)
    up_w = up_weight.reshape(2, 4 * c1, c2)
    anywhere = pl.BlockSpec(memory_space=pltpu.HBM)
    links = (11 if around else 35)
    v = pltpu.VMEM
    result = pl.pallas_call(
        functools.partial(unet, rings),
        out_shape=jax.ShapeDtypeStruct(cells.shape, F32),
        in_specs=[anywhere] * 9,
        out_specs=pl.BlockSpec(memory_space=pltpu.VMEM),
        scratch_shapes=[
            v(cells.shape, BF16), v(lift.shape, BF16), v(head_weight.shape, BF16),
            v((comps, size_z // TILE, TILE, LANES), BF16),
            v((slots, 2, comps, quarters, TILE, LANES), BF16),
            v((quarters, size_x * slots, 2 * size_y // TILE, TILE, LANES), F32),
            v((quarters, planes_d, 3 * yh, LANES), F32),
            v((comps, lift.shape[1], LANES), F32), v((depth, LANES), F32),
            v((quarters, planes_f * 2 * yh, depth), BF16),
            v((depth, quarters * LANES), BF16),
            v((comps * zw, quarters * LANES), BF16),
            v((zpairs, planes_f * 2 * yh, LANES), F32),
            v((4, planes_f, (zpairs - 2) * yh, 2 * LANES), BF16),
            v((2, zpairs - 2, yh, 2 * LANES), F32),
            v((4, planes_s, (zpairs - TILE) * TILE, 2 * LANES), BF16),
            v((4, 2 * planes_e, (zpairs - TILE) * TILE, 2 * LANES), BF16),
            v((3, planes_c, zpairs // 2 - 1, yh, 2 * LANES), BF16),
            v((3, planes_m, zpairs // 2 - 2, yh, 2 * LANES), BF16),
            v((planes_e, (zpairs // 2 - 3) * yh, 2 * LANES), BF16),
            v((2, zpairs - 6, yh, 2 * LANES), F32),
            v((size_x, 2 * TILE, LANES), F32),
            v((size_x, 2, 2 * TILE, LANES), F32),
            v((2 * LANES, 2 * LANES), F32), v((2 * LANES, 2 * LANES), BF16),
            v(encode_weight.shape, BF16), v(downward.shape, BF16), v(middle_first.shape, BF16),
            v(middle_second.shape, BF16), v(up_w.shape, BF16), v(decode_weight.shape, BF16),
            v((12, 4 * c1, 4 * c1), BF16), v((12, 4 * c1, 4 * c1), BF16),
            v((12, 4 * c1, 4 * c1), BF16),
            v((18, 2 * c2, 2 * c2), BF16), v((18, 2 * c2, 2 * c2), BF16),
            pltpu.SemaphoreType.DMA((9,)),
            pltpu.SemaphoreType.DMA((links,)), pltpu.SemaphoreType.DMA((links,)),
            pltpu.SemaphoreType.DMA((2,)),
        ],
        compiler_params=pltpu.CompilerParams(
            collective_id=0, has_side_effects=True, vmem_limit_bytes=63 * 2**20
        ),
    )(
        cells, lift, encode_weight, downward, middle_first, middle_second, up_w, decode_weight,
        head_weight,
    )
    return jnp.transpose(result, (0, 1, 3, 2))


def solution(mesh):
    placed = (P(None, "gx", "gy", "gz"), P(), P(), P(), P(), P(), P(), P(), P())
    rings = tuple(mesh.shape[axis] for axis in ("gx", "gy", "gz"))
    return jax.shard_map(
        functools.partial(local, rings), mesh=mesh, in_specs=placed,
        out_specs=P(None, "gx", "gy", "gz"), check_vma=False,
    )
```

```python
import functools

import jax
import jax.numpy as jnp
from jax import lax
from jax.experimental import pallas as pl
from jax.experimental.pallas import tpu as pltpu
from jax.sharding import PartitionSpec as P

MESH = pl.DeviceIdType.MESH
NT = (((1,), (1,)), ((), ()))
NN = (((1,), (0,)), ((), ()))
F32, BF16 = jnp.float32, jnp.bfloat16
TILE, LANES = 8, 128


def leaky(value):
    return jnp.maximum(value, 0.1 * value)


def rounded(value):
    return leaky(value).astype(BF16)


def dot(rows, weight):
    return lax.dot_general(rows, weight, NT, preferred_element_type=F32)


def build_fine(raw, wide, lo, hi):
    out = raw.shape[1]
    blank = jnp.zeros((2 * out, wide.shape[2]), BF16)
    zero = jnp.zeros((out, hi - lo), BF16)
    for a in range(3):
        wide[4 * a, 2 * out :, :] = blank
        wide[4 * a + 3, : 2 * out, :] = blank
        for b in range(3):
            taps = [raw[9 * a + 3 * b + c][:, lo:hi] for c in range(3)]
            low = jnp.concatenate([taps[1], taps[2], zero, taps[0]], axis=1)
            high = jnp.concatenate([taps[0], taps[1], taps[2], zero], axis=1)
            pair = jnp.concatenate([low, high], axis=0)
            wide[4 * a + b, : 2 * out, :] = pair
            wide[4 * a + b + 1, 2 * out :, :] = pair


def build_coarse(raw, wide):
    out = raw.shape[1]
    blank = jnp.zeros((out, raw.shape[2]), BF16)
    for a in range(3):
        for b in range(3):
            for offset in range(2):
                tile = 6 * a + 2 * b + offset
                for side in range(2):
                    for e in range(2):
                        c = 2 * offset + e - side
                        block = raw[9 * a + 3 * b + c] if 0 <= c <= 2 else blank
                        wide[tile, out * side : out * (side + 1), LANES * e : LANES * (e + 1)] = block


def unet(
    dims,
    cells_hbm, lift_hbm, encode_hbm, downward_hbm, first_hbm, second_hbm, up_hbm, decode_hbm,
    head_hbm,
    out_ref,
    cells, lift_raw, head_raw, pack, window, joint, near, spread, lift_f, lift_rows, lift_w, select_w,
    fine_in, skip_scr, skip_in, wide_in, coarse_in, middle_in, deep_scr, mine, final,
    head_f, head_w, unit,
    encode_raw, downward_w, first_raw, second_raw, up_w, decode_raw,
    encode_w, skip_w, wide_w, first_w, second_w,
    load_sems, send_sems, recv_sems, swap_sems,
):
    ring_x, ring_y, ring_z = dims
    comps, size_x, size_z, size_y = cells.shape
    around = ring_x == 2
    steps = (0,) if around else (-1, 0, 1)
    pairs = ring_x // 2
    gx, gy, gz = lax.axis_index("gx"), lax.axis_index("gy"), lax.axis_index("gz")
    mine_x, pair = lax.rem(gx, 2), lax.div(gx, 2)

    def device(step, flip, shift_y, shift_z):
        side = 1 - mine_x if flip else mine_x
        return (
            2 * lax.rem(pair + pairs + step, pairs) + side,
            lax.rem(gy + ring_y + shift_y, ring_y),
            lax.rem(gz + ring_z + shift_z, ring_z),
        )

    links = [
        (step, flip, beside, dz)
        for step in steps for flip in (0, 1) for beside in (0, 1) for dz in (-1, 0, 1)
        if (step, flip, beside, dz) != (0, 0, 0, 0)
    ]
    barrier = pltpu.get_barrier_semaphore()
    for step, flip, beside, dz in links:
        shift = 2 * mine_x - 1 if beside else 0
        pl.semaphore_signal(
            barrier, inc=1, device_id=device(step, flip, shift, -dz), device_id_type=MESH
        )
    loads = [
        pltpu.make_async_copy(src, dst, load_sems.at[i])
        for i, (src, dst) in enumerate(
            (
                (cells_hbm, cells), (lift_hbm, lift_raw), (encode_hbm, encode_raw),
                (downward_hbm, downward_w), (first_hbm, first_raw), (second_hbm, second_raw),
                (up_hbm, up_w), (decode_hbm, decode_raw), (head_hbm, head_raw),
            )
        )
    ]
    for load in loads:
        load.start()

    loads[0].wait()
    for c in range(comps):
        total = None
        for x in range(size_x):
            value = cells[c, x].astype(F32)
            value = jnp.concatenate(
                [value, jnp.zeros((size_z, LANES - size_y), F32)], axis=1
            )
            value = pltpu.roll(value, size_y * x, 1) if x else value
            total = value if total is None else total + value
        pack[c] = total.reshape(size_z // TILE, TILE, LANES).astype(BF16)
    own_slot = mine_x if around else mine_x + 2
    tiles = size_z // TILE
    window[own_slot, 1 - mine_x, :, pl.ds(1, tiles)] = pack[...]
    pl.semaphore_wait(barrier, len(links))
    copies = []
    for number, (step, flip, beside, dz) in enumerate(links):
        side = 1 - mine_x if flip else mine_x
        shift = 1 - 2 * side if beside else 0
        row_slot = side if beside else 1 - side
        slot = mine_x if around else mine_x + 2 * (step + 1)
        start, count, place = {0: (0, tiles, 1), 1: (tiles - 1, 1, 0), -1: (0, 1, tiles + 1)}[dz]
        copies.append(
            pltpu.make_async_remote_copy(
                src_ref=pack.at[:, pl.ds(start, count)],
                dst_ref=window.at[slot, row_slot, :, pl.ds(place, count)],
                send_sem=send_sems.at[number], recv_sem=recv_sems.at[number],
                device_id=device(-step, flip, shift, dz), device_id_type=MESH,
            )
        )
    for copy in copies:
        copy.start()

    loads[1].wait()
    quarters = (size_z + 2 * TILE) // TILE
    slot_lanes = LANES // quarters
    for c in range(comps):
        value = lift_raw[c].astype(F32)
        spread[c] = jnp.concatenate([value, value], axis=1)
    depth = lift_w.shape[0]
    lift_f[pl.ds(0, depth), :] = jnp.zeros((depth, LANES), F32)
    for t in range(9):
        for cz in range(3):
            for c in range(comps):
                lift_f[pl.ds(slot_lanes * t + comps * cz + c, 1), :] = spread[
                    c, pl.ds(3 * t + cz, 1), :
                ]
    base = lift_f[pl.ds(0, depth), :]
    low_half = lax.broadcasted_iota(jnp.int32, (depth, LANES), 1) < LANES // 2
    for k in range(TILE // 2):
        even = pltpu.roll(base, comps * 2 * k, 0) if k else base
        odd = pltpu.roll(base, comps * (2 * k + 1), 0)
        lift_w[:, LANES * k : LANES * (k + 1)] = jnp.where(low_half, even, odd).astype(BF16)

    rows_s, lanes_s = select_w.shape
    zw = size_z + 2 * TILE
    row = lax.broadcasted_iota(jnp.int32, (rows_s, LANES), 0)
    lane = lax.broadcasted_iota(jnp.int32, (rows_s, LANES), 1)
    place, inside = lax.div(lane, slot_lanes), lax.rem(lane, slot_lanes)
    level = lax.div(inside, comps)
    comp = inside - comps * level
    for k in range(quarters):
        source = lax.rem(place + quarters - k, quarters)
        target = comp * zw + TILE * source - 1 + level
        hit = (row == target) & (inside < comps * (TILE + 2))
        select_w[:, LANES * k : LANES * (k + 1)] = jnp.where(hit, 1.0, 0.0).astype(BF16)

    loads[2].wait()
    build_fine(encode_raw, encode_w, 0, encode_raw.shape[2])
    loads[4].wait()
    build_coarse(first_raw, first_w)
    loads[5].wait()
    build_coarse(second_raw, second_w)
    loads[7].wait()
    channels = decode_raw.shape[2] // 2
    build_fine(decode_raw, skip_w, 0, channels)
    build_fine(decode_raw, wide_w, channels, 2 * channels)
    loads[8].wait()
    head_f[...] = jnp.zeros(head_f.shape, F32)
    for p in range(2):
        for q in range(2):
            for c in range(comps):
                value = head_raw[pl.ds(c, 1), :].astype(F32)
                other = jnp.zeros_like(value)
                head_f[
                    pl.ds(LANES * p + size_z * c + q, 1), LANES * p : LANES * (p + 1)
                ] = jnp.concatenate([other, value] if q else [value, other], axis=1)
    head_w[...] = head_f[...].astype(BF16)
    unit[...] = jnp.ones(unit.shape, F32)
    loads[3].wait()
    loads[6].wait()

    for copy in copies:
        copy.wait_recv()

    slots = window.shape[0]
    turned = jnp.concatenate(
        [
            jnp.swapaxes(window[s, r].astype(F32).reshape(comps * zw, LANES), 0, 1)
            for s in range(slots) for r in range(2)
        ],
        axis=0,
    ).astype(BF16)
    grouped = lax.dot_general(turned, select_w[...], NN, preferred_element_type=F32)
    tiles_y = size_y // TILE
    for s in range(slots):
        for r in range(2):
            part = grouped[LANES * (2 * s + r) : LANES * (2 * s + r + 1)]
            for k in range(quarters):
                joint[k, pl.ds(size_x * s, size_x), pl.ds(tiles_y * r, tiles_y)] = part[
                    :, LANES * k : LANES * (k + 1)
                ].reshape(size_x, tiles_y, TILE, LANES)
    planes_d, rows_n = near.shape[1], near.shape[2]
    first_tile = tiles_y - 2 - (tiles_y // 2) * mine_x
    for k in range(quarters):
        for x in range(planes_d):
            near[k, x] = joint[k, x, pl.ds(first_tile, rows_n // TILE)].reshape(rows_n, LANES)

    planes_f = fine_in.shape[2]
    planes_c, planes_m, planes_e = coarse_in.shape[1], middle_in.shape[1], deep_scr.shape[0]
    planes_u = wide_in.shape[1]

    def source(plane, tap, total, shift=0):
        if around:
            return lax.rem(plane + tap + total - 1, total)
        return plane + tap + shift

    half_y = rows_n // 3
    slot_of = lax.div(lax.broadcasted_iota(jnp.int32, (half_y, LANES), 1), slot_lanes)

    @pl.loop(0, planes_f)
    def _(x):
        for parity in range(2):
            for q in range(quarters):
                for g in range(3):
                    taps = list(range(quarters * g, min(quarters * (g + 1), 9)))
                    value = None
                    for j, t in enumerate(taps):
                        part = near[
                            (j - q) % quarters, source(x, t // 3, planes_d),
                            pl.ds(TILE - 1 + parity + t % 3, half_y, stride=2), :,
                        ]
                        value = part if value is None else jnp.where(slot_of < j, value, part)
                    lift_rows[
                        q, pl.ds(pl.multiple_of(2 * half_y * x + half_y * parity, half_y), half_y),
                        LANES * g : LANES * (g + 1),
                    ] = value.astype(BF16)

    zpairs = zw // 2
    half = lax.broadcasted_iota(jnp.int32, (planes_f, half_y, LANES), 2) < LANES // 2
    for q in range(quarters):
        value = leaky(
            lax.dot_general(lift_rows[q], lift_w[...], NN, preferred_element_type=F32)
        )
        for r in range(quarters):
            zp = quarters * q + r
            for x in range(planes_f):
                even, odd = (
                    value[
                        half_y * (2 * x + parity) : half_y * (2 * x + parity + 1),
                        LANES * r : LANES * (r + 1),
                    ]
                    for parity in range(2)
                )
                for b, part in enumerate(
                    (pltpu.roll(odd, 1, 0), even, odd, pltpu.roll(even, half_y - 1, 0))
                ):
                    fine_in[b, zp, x, :, :LANES] = part.astype(BF16)
        for zp in range(max(quarters * q - 1, 1), quarters * q + quarters - 1):
            for b in range(4):
                fine_in[b, zp, :, :, LANES:] = jnp.where(
                    half, fine_in[b, zp + 1, :, :, :LANES], fine_in[b, zp - 1, :, :, :LANES]
                )

    inner = zpairs - 2
    quarter = TILE // 2
    own = zpairs - TILE
    low = lax.broadcasted_iota(jnp.int32, (own * TILE, LANES), 1) < LANES // 2

    def store_pairs(target, x, levels):
        for b in range(4):
            shift = quarter + (-1, 0, 0, 1)[b]
            start = LANES * ((b + 1) % 2)
            parts = [
                pltpu.roll(level[:, start : start + LANES], half_y - shift, 0)[:TILE]
                for level in levels
            ]
            plane, above, below = (
                jnp.concatenate(parts[d : d + own], axis=0) for d in (1, 2, 0)
            )
            target[b, x] = jnp.concatenate(
                [plane, jnp.where(low, above, below)], axis=1
            ).astype(BF16)

    def store_coarse(target, x, z, value):
        lanes = slice(LANES * (z % 2), LANES * (z % 2) + LANES)
        for b, part in enumerate((pltpu.roll(value, 1, 0), value, pltpu.roll(value, half_y - 1, 0))):
            target[b, x, z // 2, :, lanes] = part.astype(BF16)

    rows_e = inner * half_y

    def encode(x):
        summed = None
        for a in range(3):
            for b in range(4):
                lhs = jnp.concatenate(
                    [
                        fine_in[b, pl.ds(1, inner), source(2 * x + g, a, planes_f)].reshape(
                            rows_e, 2 * LANES
                        )
                        for g in range(2)
                    ],
                    axis=0,
                )
                term = dot(lhs, encode_w[4 * a + b])
                summed = term if summed is None else summed + term
        skip_scr[...] = rounded(summed)

    def encoded(x):
        coarse = None
        for g in range(2):
            part = skip_scr[g * rows_e : (g + 1) * rows_e]
            term = lax.dot_general(part, downward_w[g], NN, preferred_element_type=F32)
            coarse = term if coarse is None else coarse + term
        coarse = rounded(coarse).astype(F32)
        for z in range(inner):
            store_coarse(coarse_in, x, z, coarse[half_y * z : half_y * (z + 1)])
        skirt = (inner - own) // 2 - 1
        for g in range(2):
            levels = [
                skip_scr[pl.ds(g * rows_e + half_y * (skirt + z), half_y)].astype(F32)
                for z in range(own + 2)
            ]
            store_pairs(skip_in, 2 * x + g, levels)

    encode(0)

    @pl.loop(1, planes_c)
    def _(x):
        encoded(x - 1)
        encode(x)

    encoded(planes_c - 1)

    def joined(sums):
        return sums[0] + sums[1] * unit[...]

    def coarse_conv(target, weight, planes, count):
        total = target.shape[1]
        sums = [None, None]
        for a in range(3):
            for b in range(3):
                for offset in range(2):
                    lhs = jnp.concatenate(
                        [
                            target[
                                b, (x + a - 1) % total if around else x + a,
                                offset : offset + count,
                            ].reshape(count * half_y, 2 * LANES)
                            for x in range(planes)
                        ],
                        axis=0,
                    )
                    term = dot(lhs, weight[6 * a + 2 * b + offset])
                    sums[offset] = term if sums[offset] is None else sums[offset] + term
        return rounded(joined(sums))

    count = inner // 2 - 1
    middle = coarse_conv(coarse_in, first_w, planes_m, count).astype(F32)
    for x in range(planes_m):
        for z in range(2 * count):
            start = half_y * (count * x + z // 2)
            store_coarse(
                middle_in, x, z,
                middle[start : start + half_y, LANES * (z % 2) : LANES * (z % 2) + LANES],
            )
    count -= 1
    deep = coarse_conv(middle_in, second_w, planes_e, count)
    deep_scr[...] = deep.reshape(planes_e, count * half_y, 2 * LANES)

    for x in range(planes_e):
        sides = [deep_scr[x, :, LANES * side : LANES * (side + 1)] for side in range(2)]
        for a in range(2):
            values = [rounded(dot(lhs, up_w[a])).astype(F32) for lhs in sides]
            levels = [
                values[z % 2][half_y * (z // 2) : half_y * (z // 2 + 1)] for z in range(own + 2)
            ]
            store_pairs(wide_in, 2 * x + a, levels)

    swap = None
    for turn in range(2):
        side = mine_x if turn else 1 - mine_x
        sums = [None, None]
        for array, weight, shift in ((skip_in, skip_w, 5), (wide_in, wide_w, 1)):
            total = array.shape[1]
            for a in range(3):
                for b in range(4):
                    lhs = jnp.concatenate(
                        [
                            array[b, source(size_x * side + g, a, total, shift)]
                            for g in range(size_x)
                        ],
                        axis=0,
                    )
                    term = dot(lhs, weight[4 * a + b])
                    sums[b % 2] = term if sums[b % 2] is None else sums[b % 2] + term
        result = dot(rounded(joined(sums)), head_w[...])
        for g in range(size_x):
            for p in range(2):
                total = None
                for z in range(own):
                    start = TILE * (own * g + z)
                    value = result[start : start + TILE, LANES * p : LANES * (p + 1)]
                    value = pltpu.roll(value, 2 * z, 1) if z else value
                    total = value if total is None else total + value
                if turn:
                    final[g, mine_x, pl.ds(p, TILE, stride=2), :] = total
                else:
                    mine[g, pl.ds(p, TILE, stride=2), :] = total
        if not turn:
            swap = pltpu.make_async_remote_copy(
                src_ref=mine, dst_ref=final.at[:, mine_x],
                send_sem=swap_sems.at[0], recv_sem=swap_sems.at[1],
                device_id=device(0, 1, 0, 0), device_id_type=MESH,
            )
            swap.start()
    swap.wait_recv()
    flat = jnp.swapaxes(final[...].reshape(LANES, LANES), 0, 1)
    for c in range(comps):
        block = flat[size_z * c : size_z * (c + 1)]
        for x in range(size_x):
            value = pltpu.roll(block, LANES - size_y * x, 1) if x else block
            out_ref[c, x] = cells[c, x].astype(F32) + value[:, :size_y]
    for copy in copies:
        copy.wait_send()
    swap.wait_send()


def local(
    rings, displacement, lift_weight, encode_weight, downward_weight, middle_first, middle_second,
    up_weight, decode_weight, head_weight,
):
    comps, size_x, size_y, size_z = displacement.shape
    c1, c2 = encode_weight.shape[1], middle_first.shape[1]
    around = rings[0] == 2
    slots = 2 if around else 6
    span = 2 * size_x
    halo = (lambda h: 0) if around else (lambda h: h)
    zw, yh = size_z + 2 * TILE, (size_y // 2 + 2 * TILE) // 2
    zpairs, quarters = zw // 2, zw // TILE
    planes_d, planes_f, planes_s = (span + 2 * halo(h) for h in (8, 7, 6))
    planes_c, planes_m, planes_e = (span // 2 + 2 * halo(h) for h in (3, 2, 1))
    depth = 3 * LANES

    cells = jnp.transpose(displacement, (0, 1, 3, 2))
    lift = jnp.transpose(lift_weight, (2, 0, 1))
    downward = jnp.transpose(downward_weight, (0, 2, 1)).reshape(2, 4 * c1, c2)
    up_w = up_weight.reshape(2, 4 * c1, c2)
    anywhere = pl.BlockSpec(memory_space=pltpu.HBM)
    links = (11 if around else 35)
    v = pltpu.VMEM
    result = pl.pallas_call(
        functools.partial(unet, rings),
        out_shape=pltpu.VMEM(cells.shape, F32),
        in_specs=[anywhere] * 9,
        out_specs=pl.BlockSpec(memory_space=pltpu.VMEM),
        scratch_shapes=[
            v(cells.shape, BF16), v(lift.shape, BF16), v(head_weight.shape, BF16),
            v((comps, size_z // TILE, TILE, LANES), BF16),
            v((slots, 2, comps, quarters, TILE, LANES), BF16),
            v((quarters, size_x * slots, 2 * size_y // TILE, TILE, LANES), F32),
            v((quarters, planes_d, 3 * yh, LANES), F32),
            v((comps, lift.shape[1], LANES), F32), v((depth, LANES), F32),
            v((quarters, planes_f * 2 * yh, depth), BF16),
            v((depth, quarters * LANES), BF16),
            v((comps * zw, quarters * LANES), BF16),
            v((4, zpairs, planes_f, yh, 2 * LANES), BF16),
            v((2 * (zpairs - 2) * yh, 2 * LANES), BF16),
            v((4, planes_s, (zpairs - TILE) * TILE, 2 * LANES), BF16),
            v((4, 2 * planes_e, (zpairs - TILE) * TILE, 2 * LANES), BF16),
            v((3, planes_c, zpairs // 2 - 1, yh, 2 * LANES), BF16),
            v((3, planes_m, zpairs // 2 - 2, yh, 2 * LANES), BF16),
            v((planes_e, (zpairs // 2 - 3) * yh, 2 * LANES), BF16),
            v((size_x, 2 * TILE, LANES), F32),
            v((size_x, 2, 2 * TILE, LANES), F32),
            v((2 * LANES, 2 * LANES), F32), v((2 * LANES, 2 * LANES), BF16), v((1, 2 * LANES), F32),
            v(encode_weight.shape, BF16), v(downward.shape, BF16), v(middle_first.shape, BF16),
            v(middle_second.shape, BF16), v(up_w.shape, BF16), v(decode_weight.shape, BF16),
            v((12, 4 * c1, 4 * c1), BF16), v((12, 4 * c1, 4 * c1), BF16),
            v((12, 4 * c1, 4 * c1), BF16),
            v((18, 2 * c2, 2 * c2), BF16), v((18, 2 * c2, 2 * c2), BF16),
            pltpu.SemaphoreType.DMA((9,)),
            pltpu.SemaphoreType.DMA((links,)), pltpu.SemaphoreType.DMA((links,)),
            pltpu.SemaphoreType.DMA((2,)),
        ],
        compiler_params=pltpu.CompilerParams(
            collective_id=0, has_side_effects=True, vmem_limit_bytes=63 * 2**20
        ),
    )(
        cells, lift, encode_weight, downward, middle_first, middle_second, up_w, decode_weight,
        head_weight,
    )
    return jnp.transpose(result, (0, 1, 3, 2))


def solution(mesh):
    placed = (P(None, "gx", "gy", "gz"), P(), P(), P(), P(), P(), P(), P(), P())
    rings = tuple(mesh.shape[axis] for axis in ("gx", "gy", "gz"))
    return jax.shard_map(
        functools.partial(local, rings), mesh=mesh, in_specs=placed,
        out_specs=P(None, "gx", "gy", "gz"), check_vma=False,
    )
```

```python
import functools

import jax
import jax.numpy as jnp
from jax import lax
from jax.experimental import pallas as pl
from jax.experimental.pallas import tpu as pltpu
from jax.sharding import PartitionSpec as P

MESH = pl.DeviceIdType.MESH
NT = (((1,), (1,)), ((), ()))
NN = (((1,), (0,)), ((), ()))
F32, BF16 = jnp.float32, jnp.bfloat16
TILE, LANES = 8, 128


def leaky(value):
    return jnp.maximum(value, 0.1 * value)


def rounded(value):
    return leaky(value).astype(BF16)


def dot(rows, weight):
    return lax.dot_general(rows, weight, NT, preferred_element_type=F32)


def build_fine(raw, wide, lo, hi):
    out = raw.shape[1]
    blank = jnp.zeros((2 * out, wide.shape[2]), BF16)
    zero = jnp.zeros((out, hi - lo), BF16)
    for a in range(3):
        wide[4 * a, 2 * out :, :] = blank
        wide[4 * a + 3, : 2 * out, :] = blank
        for b in range(3):
            taps = [raw[9 * a + 3 * b + c][:, lo:hi] for c in range(3)]
            low = jnp.concatenate([taps[1], taps[2], zero, taps[0]], axis=1)
            high = jnp.concatenate([taps[0], taps[1], taps[2], zero], axis=1)
            pair = jnp.concatenate([low, high], axis=0)
            wide[4 * a + b, : 2 * out, :] = pair
            wide[4 * a + b + 1, 2 * out :, :] = pair


def build_coarse(raw, wide):
    out = raw.shape[1]
    blank = jnp.zeros((out, raw.shape[2]), BF16)
    for a in range(3):
        for b in range(3):
            for offset in range(2):
                tile = 6 * a + 2 * b + offset
                for side in range(2):
                    for e in range(2):
                        c = 2 * offset + e - side
                        block = raw[9 * a + 3 * b + c] if 0 <= c <= 2 else blank
                        wide[tile, out * side : out * (side + 1), LANES * e : LANES * (e + 1)] = block


def unet(
    dims,
    cells_hbm, lift_hbm, encode_hbm, downward_hbm, first_hbm, second_hbm, up_hbm, decode_hbm,
    head_hbm,
    out_ref,
    cells, lift_raw, head_raw, pack, window, joint, near, spread, lift_f, lift_rows, lift_w, select_w,
    fine_in, skip_two, skip_in, wide_in, coarse_in, middle_in, deep_scr, mine, final, ahead,
    head_f, head_w, unit,
    encode_raw, downward_w, first_raw, second_raw, up_w, decode_raw,
    encode_w, skip_w, wide_w, first_w, second_w,
    load_sems, send_sems, recv_sems, swap_sems,
):
    ring_x, ring_y, ring_z = dims
    comps, size_x, size_z, size_y = cells.shape
    around = ring_x == 2
    steps = (0,) if around else (-1, 0, 1)
    pairs = ring_x // 2
    gx, gy, gz = lax.axis_index("gx"), lax.axis_index("gy"), lax.axis_index("gz")
    mine_x, pair = lax.rem(gx, 2), lax.div(gx, 2)

    def device(step, flip, shift_y, shift_z):
        side = 1 - mine_x if flip else mine_x
        return (
            2 * lax.rem(pair + pairs + step, pairs) + side,
            lax.rem(gy + ring_y + shift_y, ring_y),
            lax.rem(gz + ring_z + shift_z, ring_z),
        )

    links = [
        (step, flip, beside, dz)
        for step in steps for flip in (0, 1) for beside in (0, 1) for dz in (-1, 0, 1)
        if (step, flip, beside, dz) != (0, 0, 0, 0)
    ]
    barrier = pltpu.get_barrier_semaphore()
    for step, flip, beside, dz in links:
        shift = 2 * mine_x - 1 if beside else 0
        pl.semaphore_signal(
            barrier, inc=1, device_id=device(step, flip, shift, -dz), device_id_type=MESH
        )
    loads = [
        pltpu.make_async_copy(src, dst, load_sems.at[i])
        for i, (src, dst) in enumerate(
            (
                (cells_hbm, cells), (lift_hbm, lift_raw), (encode_hbm, encode_raw),
                (downward_hbm, downward_w), (first_hbm, first_raw), (second_hbm, second_raw),
                (up_hbm, up_w), (decode_hbm, decode_raw), (head_hbm, head_raw),
            )
        )
    ]
    for load in loads:
        load.start()

    loads[0].wait()
    for c in range(comps):
        total = None
        for x in range(size_x):
            value = cells[c, x].astype(F32)
            value = jnp.concatenate(
                [value, jnp.zeros((size_z, LANES - size_y), F32)], axis=1
            )
            value = pltpu.roll(value, size_y * x, 1) if x else value
            total = value if total is None else total + value
        pack[c] = total.reshape(size_z // TILE, TILE, LANES).astype(BF16)
    own_slot = mine_x if around else mine_x + 2
    tiles = size_z // TILE
    window[own_slot, 1 - mine_x, :, pl.ds(1, tiles)] = pack[...]
    pl.semaphore_wait(barrier, len(links))
    copies = []
    for number, (step, flip, beside, dz) in enumerate(links):
        side = 1 - mine_x if flip else mine_x
        shift = 1 - 2 * side if beside else 0
        row_slot = side if beside else 1 - side
        slot = mine_x if around else mine_x + 2 * (step + 1)
        start, count, place = {0: (0, tiles, 1), 1: (tiles - 1, 1, 0), -1: (0, 1, tiles + 1)}[dz]
        copies.append(
            pltpu.make_async_remote_copy(
                src_ref=pack.at[:, pl.ds(start, count)],
                dst_ref=window.at[slot, row_slot, :, pl.ds(place, count)],
                send_sem=send_sems.at[number], recv_sem=recv_sems.at[number],
                device_id=device(-step, flip, shift, dz), device_id_type=MESH,
            )
        )
    for copy in copies:
        copy.start()

    loads[1].wait()
    quarters = (size_z + 2 * TILE) // TILE
    slot_lanes = LANES // quarters
    for c in range(comps):
        value = lift_raw[c].astype(F32)
        spread[c] = jnp.concatenate([value, value], axis=1)
    depth = lift_w.shape[0]
    lift_f[pl.ds(0, depth), :] = jnp.zeros((depth, LANES), F32)
    for t in range(9):
        for cz in range(3):
            for c in range(comps):
                lift_f[pl.ds(slot_lanes * t + comps * cz + c, 1), :] = spread[
                    c, pl.ds(3 * t + cz, 1), :
                ]
    base = lift_f[pl.ds(0, depth), :]
    low_half = lax.broadcasted_iota(jnp.int32, (depth, LANES), 1) < LANES // 2
    for k in range(TILE // 2):
        even = pltpu.roll(base, comps * 2 * k, 0) if k else base
        odd = pltpu.roll(base, comps * (2 * k + 1), 0)
        lift_w[:, LANES * k : LANES * (k + 1)] = jnp.where(low_half, even, odd).astype(BF16)

    rows_s, lanes_s = select_w.shape
    zw = size_z + 2 * TILE
    row = lax.broadcasted_iota(jnp.int32, (rows_s, LANES), 0)
    lane = lax.broadcasted_iota(jnp.int32, (rows_s, LANES), 1)
    place, inside = lax.div(lane, slot_lanes), lax.rem(lane, slot_lanes)
    level = lax.div(inside, comps)
    comp = inside - comps * level
    for k in range(quarters):
        source = lax.rem(place + quarters - k, quarters)
        target = comp * zw + TILE * source - 1 + level
        hit = (row == target) & (inside < comps * (TILE + 2))
        select_w[:, LANES * k : LANES * (k + 1)] = jnp.where(hit, 1.0, 0.0).astype(BF16)

    loads[2].wait()
    build_fine(encode_raw, encode_w, 0, encode_raw.shape[2])
    loads[4].wait()
    build_coarse(first_raw, first_w)
    loads[5].wait()
    build_coarse(second_raw, second_w)
    loads[7].wait()
    channels = decode_raw.shape[2] // 2
    build_fine(decode_raw, skip_w, 0, channels)
    build_fine(decode_raw, wide_w, channels, 2 * channels)
    loads[8].wait()
    head_f[...] = jnp.zeros(head_f.shape, F32)
    for p in range(2):
        for q in range(2):
            for c in range(comps):
                value = head_raw[pl.ds(c, 1), :].astype(F32)
                other = jnp.zeros_like(value)
                head_f[
                    pl.ds(LANES * p + size_z * c + q, 1), LANES * p : LANES * (p + 1)
                ] = jnp.concatenate([other, value] if q else [value, other], axis=1)
    head_w[...] = head_f[...].astype(BF16)
    unit[...] = jnp.ones(unit.shape, F32)
    loads[3].wait()
    loads[6].wait()

    for copy in copies:
        copy.wait_recv()

    slots = window.shape[0]
    turned = jnp.concatenate(
        [
            jnp.swapaxes(window[s, r].astype(F32).reshape(comps * zw, LANES), 0, 1)
            for s in range(slots) for r in range(2)
        ],
        axis=0,
    ).astype(BF16)
    grouped = lax.dot_general(turned, select_w[...], NN, preferred_element_type=F32)
    tiles_y = size_y // TILE
    for s in range(slots):
        for r in range(2):
            part = grouped[LANES * (2 * s + r) : LANES * (2 * s + r + 1)]
            for k in range(quarters):
                joint[k, pl.ds(size_x * s, size_x), pl.ds(tiles_y * r, tiles_y)] = part[
                    :, LANES * k : LANES * (k + 1)
                ].reshape(size_x, tiles_y, TILE, LANES)
    planes_d, rows_n = near.shape[1], near.shape[2]
    first_tile = tiles_y - 2 - (tiles_y // 2) * mine_x
    for k in range(quarters):
        for x in range(planes_d):
            near[k, x] = joint[k, x, pl.ds(first_tile, rows_n // TILE)].reshape(rows_n, LANES)

    planes_f = fine_in.shape[2]
    planes_c, planes_m, planes_e = coarse_in.shape[1], middle_in.shape[1], deep_scr.shape[0]
    planes_u = wide_in.shape[1]

    def source(plane, tap, total, shift=0):
        if around:
            if isinstance(plane, int):
                return (plane + tap - 1) % total
            return lax.rem(plane + tap + total - 1, total)
        return plane + tap + shift

    half_y = rows_n // 3
    slot_of = lax.div(lax.broadcasted_iota(jnp.int32, (half_y, LANES), 1), slot_lanes)

    @pl.loop(0, planes_f)
    def _(x):
        for parity in range(2):
            for q in range(quarters):
                for g in range(3):
                    taps = list(range(quarters * g, min(quarters * (g + 1), 9)))
                    value = None
                    for j, t in enumerate(taps):
                        part = near[
                            (j - q) % quarters, source(x, t // 3, planes_d),
                            pl.ds(TILE - 1 + parity + t % 3, half_y, stride=2), :,
                        ]
                        value = part if value is None else jnp.where(slot_of < j, value, part)
                    lift_rows[
                        q, pl.ds(pl.multiple_of(2 * half_y * x + half_y * parity, half_y), half_y),
                        LANES * g : LANES * (g + 1),
                    ] = value.astype(BF16)

    zpairs = zw // 2
    half = lax.broadcasted_iota(jnp.int32, (planes_f, half_y, LANES), 2) < LANES // 2
    for q in range(quarters):
        value = leaky(
            lax.dot_general(lift_rows[q], lift_w[...], NN, preferred_element_type=F32)
        )
        for r in range(quarters):
            zp = quarters * q + r
            for x in range(planes_f):
                even, odd = (
                    value[
                        half_y * (2 * x + parity) : half_y * (2 * x + parity + 1),
                        LANES * r : LANES * (r + 1),
                    ]
                    for parity in range(2)
                )
                for b, part in enumerate(
                    (pltpu.roll(odd, 1, 0), even, odd, pltpu.roll(even, half_y - 1, 0))
                ):
                    fine_in[b, zp, x, :, :LANES] = part.astype(BF16)
        for zp in range(max(quarters * q - 1, 1), quarters * q + quarters - 1):
            for b in range(4):
                fine_in[b, zp, :, :, LANES:] = jnp.where(
                    half, fine_in[b, zp + 1, :, :, :LANES], fine_in[b, zp - 1, :, :, :LANES]
                )

    inner = zpairs - 2
    quarter = TILE // 2
    own = zpairs - TILE
    low = lax.broadcasted_iota(jnp.int32, (own * TILE, LANES), 1) < LANES // 2

    def store_pairs(target, x, levels):
        for b in range(4):
            shift = quarter + (-1, 0, 0, 1)[b]
            start = LANES * ((b + 1) % 2)
            parts = [
                pltpu.roll(level[:, start : start + LANES], half_y - shift, 0)[:TILE]
                for level in levels
            ]
            plane, above, below = (
                jnp.concatenate(parts[d : d + own], axis=0) for d in (1, 2, 0)
            )
            target[b, x] = jnp.concatenate(
                [plane, jnp.where(low, above, below)], axis=1
            ).astype(BF16)

    def store_coarse(target, x, z, value):
        lanes = slice(LANES * (z % 2), LANES * (z % 2) + LANES)
        for b, part in enumerate((pltpu.roll(value, 1, 0), value, pltpu.roll(value, half_y - 1, 0))):
            target[b, x, z // 2, :, lanes] = part.astype(BF16)

    rows_e = inner * half_y

    def joined(sums):
        return sums[0] + sums[1] * unit[...]

    def encode(x):
        skip_scr = skip_two.at[x % 2]
        sums = [None, None]
        for a in range(3):
            for b in range(4):
                lhs = jnp.concatenate(
                    [
                        fine_in[b, pl.ds(1, inner), source(2 * x + g, a, planes_f)].reshape(
                            rows_e, 2 * LANES
                        )
                        for g in range(2)
                    ],
                    axis=0,
                )
                term = dot(lhs, encode_w[4 * a + b])
                sums[b % 2] = term if sums[b % 2] is None else sums[b % 2] + term
        skip_scr[...] = rounded(joined(sums))

    def encoded(x):
        skip_scr = skip_two.at[x % 2]
        coarse = None
        for g in range(2):
            part = skip_scr[g * rows_e : (g + 1) * rows_e]
            term = lax.dot_general(part, downward_w[g], NN, preferred_element_type=F32)
            coarse = term if coarse is None else coarse + term
        coarse = rounded(coarse).astype(F32)
        for z in range(inner):
            store_coarse(coarse_in, x, z, coarse[half_y * z : half_y * (z + 1)])

    def kept(x):
        skip_scr = skip_two.at[x % 2]
        skirt = (inner - own) // 2 - 1
        for g in range(2):
            levels = [
                skip_scr[pl.ds(g * rows_e + half_y * (skirt + z), half_y)].astype(F32)
                for z in range(own + 2)
            ]
            store_pairs(skip_in, 2 * x + g, levels)

    encode(0)

    for x in range(1, planes_c):
        encode(x)
        encoded(x - 1)
        kept(x - 1)

    encoded(planes_c - 1)

    def coarse_conv(target, weight, planes, count):
        total = target.shape[1]
        sums = [None, None]
        for a in range(3):
            for b in range(3):
                for offset in range(2):
                    lhs = jnp.concatenate(
                        [
                            target[
                                b, (x + a - 1) % total if around else x + a,
                                offset : offset + count,
                            ].reshape(count * half_y, 2 * LANES)
                            for x in range(planes)
                        ],
                        axis=0,
                    )
                    term = dot(lhs, weight[6 * a + 2 * b + offset])
                    sums[offset] = term if sums[offset] is None else sums[offset] + term
        return joined(sums)

    def decode(array, weight, side, shift, taps):
        sums = [None, None]
        for number, (a, b) in enumerate(taps):
            lhs = jnp.concatenate(
                [
                    array[b, source(size_x * side + g, a, array.shape[1], shift)]
                    for g in range(size_x)
                ],
                axis=0,
            )
            term = dot(lhs, weight[4 * a + b])
            n = number % 2
            sums[n] = term if sums[n] is None else sums[n] + term
        return joined(sums)

    taps = [(a, b) for a in range(3) for b in range(4)]
    count = inner // 2 - 1
    middle = coarse_conv(coarse_in, first_w, planes_m, count)
    kept(planes_c - 1)
    ahead[...] = decode(skip_in, skip_w, 1 - mine_x, 5, taps[:6])
    middle = rounded(middle).astype(F32)
    for x in range(planes_m):
        for z in range(2 * count):
            start = half_y * (count * x + z // 2)
            store_coarse(
                middle_in, x, z,
                middle[start : start + half_y, LANES * (z % 2) : LANES * (z % 2) + LANES],
            )
    count -= 1
    deep = coarse_conv(middle_in, second_w, planes_e, count)
    ahead[...] += decode(skip_in, skip_w, 1 - mine_x, 5, taps[6:])
    deep_scr[...] = rounded(deep).reshape(planes_e, count * half_y, 2 * LANES)

    for x in range(planes_e):
        sides = [deep_scr[x, :, LANES * side : LANES * (side + 1)] for side in range(2)]
        for a in range(2):
            values = [rounded(dot(lhs, up_w[a])).astype(F32) for lhs in sides]
            levels = [
                values[z % 2][half_y * (z // 2) : half_y * (z // 2 + 1)] for z in range(own + 2)
            ]
            store_pairs(wide_in, 2 * x + a, levels)

    swap = None
    for turn in range(2):
        side = mine_x if turn else 1 - mine_x
        if turn:
            ahead[...] = decode(skip_in, skip_w, side, 5, taps)
        summed = ahead[...] + decode(wide_in, wide_w, side, 1, taps)
        result = dot(rounded(summed), head_w[...])
        for p in range(2):
            totals = []
            for g in range(size_x):
                total = None
                for z in range(own):
                    start = TILE * (own * g + z)
                    value = result[start : start + TILE, LANES * p : LANES * (p + 1)]
                    value = pltpu.roll(value, 2 * z, 1) if z else value
                    total = value if total is None else total + value
                totals.append(total)
            for g in range(size_x // 2):
                total = totals[g] + pltpu.roll(totals[g + size_x // 2], LANES // 2, 1)
                if turn:
                    final[g, mine_x, pl.ds(p, TILE, stride=2), :] = total
                else:
                    mine[g, pl.ds(p, TILE, stride=2), :] = total
        if not turn:
            swap = pltpu.make_async_remote_copy(
                src_ref=mine, dst_ref=final.at[:, mine_x],
                send_sem=swap_sems.at[0], recv_sem=swap_sems.at[1],
                device_id=device(0, 1, 0, 0), device_id_type=MESH,
            )
            swap.start()
    swap.wait_recv()
    flat = jnp.swapaxes(final[...].reshape(LANES // 2, LANES), 0, 1)
    for c in range(comps):
        for x in range(size_x):
            start = LANES // 2 * (2 * x // size_x) + size_z * c
            shift = size_y * (x % (size_x // 2))
            out_ref[c, x] = cells[c, x].astype(F32) + flat[
                start : start + size_z, shift : shift + size_y
            ]
    for copy in copies:
        copy.wait_send()
    swap.wait_send()


def local(
    rings, displacement, lift_weight, encode_weight, downward_weight, middle_first, middle_second,
    up_weight, decode_weight, head_weight,
):
    comps, size_x, size_y, size_z = displacement.shape
    c1, c2 = encode_weight.shape[1], middle_first.shape[1]
    around = rings[0] == 2
    slots = 2 if around else 6
    span = 2 * size_x
    halo = (lambda h: 0) if around else (lambda h: h)
    zw, yh = size_z + 2 * TILE, (size_y // 2 + 2 * TILE) // 2
    zpairs, quarters = zw // 2, zw // TILE
    planes_d, planes_f, planes_s = (span + 2 * halo(h) for h in (8, 7, 6))
    planes_c, planes_m, planes_e = (span // 2 + 2 * halo(h) for h in (3, 2, 1))
    depth = 3 * LANES

    cells = jnp.transpose(displacement, (0, 1, 3, 2))
    lift = jnp.transpose(lift_weight, (2, 0, 1))
    downward = jnp.transpose(downward_weight, (0, 2, 1)).reshape(2, 4 * c1, c2)
    up_w = up_weight.reshape(2, 4 * c1, c2)
    anywhere = pl.BlockSpec(memory_space=pltpu.HBM)
    links = (11 if around else 35)
    v = pltpu.VMEM
    result = pl.pallas_call(
        functools.partial(unet, rings),
        out_shape=pltpu.VMEM(cells.shape, F32),
        in_specs=[anywhere] * 9,
        out_specs=pl.BlockSpec(memory_space=pltpu.VMEM),
        scratch_shapes=[
            v(cells.shape, BF16), v(lift.shape, BF16), v(head_weight.shape, BF16),
            v((comps, size_z // TILE, TILE, LANES), BF16),
            v((slots, 2, comps, quarters, TILE, LANES), BF16),
            v((quarters, size_x * slots, 2 * size_y // TILE, TILE, LANES), F32),
            v((quarters, planes_d, 3 * yh, LANES), F32),
            v((comps, lift.shape[1], LANES), F32), v((depth, LANES), F32),
            v((quarters, planes_f * 2 * yh, depth), BF16),
            v((depth, quarters * LANES), BF16),
            v((comps * zw, quarters * LANES), BF16),
            v((4, zpairs, planes_f, yh, 2 * LANES), BF16),
            v((2, 2 * (zpairs - 2) * yh, 2 * LANES), BF16),
            v((4, planes_s, (zpairs - TILE) * TILE, 2 * LANES), BF16),
            v((4, 2 * planes_e, (zpairs - TILE) * TILE, 2 * LANES), BF16),
            v((3, planes_c, zpairs // 2 - 1, yh, 2 * LANES), BF16),
            v((3, planes_m, zpairs // 2 - 2, yh, 2 * LANES), BF16),
            v((planes_e, (zpairs // 2 - 3) * yh, 2 * LANES), BF16),
            v((size_x // 2, 2 * TILE, LANES), F32),
            v((size_x // 2, 2, 2 * TILE, LANES), F32),
            v((size_x * (zpairs - TILE) * TILE, 2 * LANES), F32),
            v((2 * LANES, 2 * LANES), F32), v((2 * LANES, 2 * LANES), BF16), v((1, 2 * LANES), F32),
            v(encode_weight.shape, BF16), v(downward.shape, BF16), v(middle_first.shape, BF16),
            v(middle_second.shape, BF16), v(up_w.shape, BF16), v(decode_weight.shape, BF16),
            v((12, 4 * c1, 4 * c1), BF16), v((12, 4 * c1, 4 * c1), BF16),
            v((12, 4 * c1, 4 * c1), BF16),
            v((18, 2 * c2, 2 * c2), BF16), v((18, 2 * c2, 2 * c2), BF16),
            pltpu.SemaphoreType.DMA((9,)),
            pltpu.SemaphoreType.DMA((links,)), pltpu.SemaphoreType.DMA((links,)),
            pltpu.SemaphoreType.DMA((2,)),
        ],
        compiler_params=pltpu.CompilerParams(
            collective_id=0, has_side_effects=True, vmem_limit_bytes=63 * 2**20
        ),
    )(
        cells, lift, encode_weight, downward, middle_first, middle_second, up_w, decode_weight,
        head_weight,
    )
    return jnp.transpose(result, (0, 1, 3, 2))


def solution(mesh):
    placed = (P(None, "gx", "gy", "gz"), P(), P(), P(), P(), P(), P(), P(), P())
    rings = tuple(mesh.shape[axis] for axis in ("gx", "gy", "gz"))
    return jax.shard_map(
        functools.partial(local, rings), mesh=mesh, in_specs=placed,
        out_specs=P(None, "gx", "gy", "gz"), check_vma=False,
    )
```

```python
import functools

import jax
import jax.numpy as jnp
from jax import lax
from jax.experimental import pallas as pl
from jax.experimental.pallas import tpu as pltpu
from jax.sharding import PartitionSpec as P

MESH = pl.DeviceIdType.MESH
NT = (((1,), (1,)), ((), ()))
NN = (((1,), (0,)), ((), ()))
F32, BF16 = jnp.float32, jnp.bfloat16
TILE, LANES = 8, 128


def leaky(value):
    return jnp.maximum(value, 0.1 * value)


def rounded(value):
    return leaky(value).astype(BF16)


def dot(rows, weight):
    return lax.dot_general(rows, weight, NT, preferred_element_type=F32)


def build_fine(raw, wide, lo, hi, odd=False):
    out = raw.shape[1]
    blank = jnp.zeros((2 * out, wide.shape[2]), BF16)
    zero = jnp.zeros((out, hi - lo), BF16)
    for a in range(3):
        wide[4 * a, 2 * out :, :] = blank
        wide[4 * a + 3, : 2 * out, :] = blank
        for b in range(3):
            taps = [raw[9 * a + 3 * b + c][:, lo:hi] for c in range(3)]
            if odd:
                low = jnp.concatenate([taps[0], taps[1], taps[2], zero], axis=1)
                high = jnp.concatenate([zero, taps[0], taps[1], taps[2]], axis=1)
            else:
                low = jnp.concatenate([taps[1], taps[2], zero, taps[0]], axis=1)
                high = jnp.concatenate([taps[0], taps[1], taps[2], zero], axis=1)
            pair = jnp.concatenate([low, high], axis=0)
            wide[4 * a + b, : 2 * out, :] = pair
            wide[4 * a + b + 1, 2 * out :, :] = pair


def build_coarse(raw, wide):
    out = raw.shape[1]
    blank = jnp.zeros((out, raw.shape[2]), BF16)
    for a in range(3):
        for b in range(3):
            for offset in range(2):
                tile = 6 * a + 2 * b + offset
                for side in range(2):
                    for e in range(2):
                        c = 2 * offset + e - side
                        block = raw[9 * a + 3 * b + c] if 0 <= c <= 2 else blank
                        wide[tile, out * side : out * (side + 1), LANES * e : LANES * (e + 1)] = block


def unet(
    dims,
    cells_hbm, lift_hbm, encode_hbm, downward_hbm, first_hbm, second_hbm, up_hbm, decode_hbm,
    head_hbm,
    out_ref,
    cells, lift_raw, head_raw, pack, window, joint, near, spread, lift_f, lift_rows, lift_w, select_w,
    fine_in, skip_two, skip_in, wide_in, coarse_in, middle_in, deep_scr, mine, final, ahead,
    head_f, head_w, unit,
    encode_raw, downward_w, first_raw, second_raw, up_w, decode_raw,
    encode_w, skip_w, wide_w, first_w, second_w,
    load_sems, send_sems, recv_sems, swap_sems,
):
    ring_x, ring_y, ring_z = dims
    comps, size_x, size_z, size_y = cells.shape
    around = ring_x == 2
    steps = (0,) if around else (-1, 0, 1)
    pairs = ring_x // 2
    gx, gy, gz = lax.axis_index("gx"), lax.axis_index("gy"), lax.axis_index("gz")
    mine_x, pair = lax.rem(gx, 2), lax.div(gx, 2)

    def device(step, flip, shift_y, shift_z):
        side = 1 - mine_x if flip else mine_x
        return (
            2 * lax.rem(pair + pairs + step, pairs) + side,
            lax.rem(gy + ring_y + shift_y, ring_y),
            lax.rem(gz + ring_z + shift_z, ring_z),
        )

    links = [
        (step, flip, beside, dz)
        for step in steps for flip in (0, 1) for beside in (0, 1) for dz in (-1, 0, 1)
        if (step, flip, beside, dz) != (0, 0, 0, 0)
    ]
    barrier = pltpu.get_barrier_semaphore()
    for step, flip, beside, dz in links:
        shift = 2 * mine_x - 1 if beside else 0
        pl.semaphore_signal(
            barrier, inc=1, device_id=device(step, flip, shift, -dz), device_id_type=MESH
        )
    loads = [
        pltpu.make_async_copy(src, dst, load_sems.at[i])
        for i, (src, dst) in enumerate(
            (
                (cells_hbm, cells), (lift_hbm, lift_raw), (encode_hbm, encode_raw),
                (downward_hbm, downward_w), (first_hbm, first_raw), (second_hbm, second_raw),
                (up_hbm, up_w), (decode_hbm, decode_raw), (head_hbm, head_raw),
            )
        )
    ]
    for load in loads:
        load.start()

    loads[0].wait()
    for c in range(comps):
        total = None
        for x in range(size_x):
            value = cells[c, x].astype(F32)
            value = jnp.concatenate(
                [value, jnp.zeros((size_z, LANES - size_y), F32)], axis=1
            )
            value = pltpu.roll(value, size_y * x, 1) if x else value
            total = value if total is None else total + value
        pack[c] = total.reshape(size_z // TILE, TILE, LANES).astype(BF16)
    own_slot = mine_x if around else mine_x + 2
    tiles = size_z // TILE
    window[own_slot, 1 - mine_x, :, pl.ds(1, tiles)] = pack[...]
    pl.semaphore_wait(barrier, len(links))
    copies = []
    for number, (step, flip, beside, dz) in enumerate(links):
        side = 1 - mine_x if flip else mine_x
        shift = 1 - 2 * side if beside else 0
        row_slot = side if beside else 1 - side
        slot = mine_x if around else mine_x + 2 * (step + 1)
        start, count, place = {0: (0, tiles, 1), 1: (tiles - 1, 1, 0), -1: (0, 1, tiles + 1)}[dz]
        copies.append(
            pltpu.make_async_remote_copy(
                src_ref=pack.at[:, pl.ds(start, count)],
                dst_ref=window.at[slot, row_slot, :, pl.ds(place, count)],
                send_sem=send_sems.at[number], recv_sem=recv_sems.at[number],
                device_id=device(-step, flip, shift, dz), device_id_type=MESH,
            )
        )
    for copy in copies:
        copy.start()

    loads[1].wait()
    quarters = (size_z + 2 * TILE) // TILE
    slot_lanes = LANES // quarters
    for c in range(comps):
        value = lift_raw[c].astype(F32)
        spread[c] = jnp.concatenate([value, value], axis=1)
    depth = lift_w.shape[0]
    lift_f[pl.ds(0, depth), :] = jnp.zeros((depth, LANES), F32)
    for t in range(9):
        for cz in range(3):
            for c in range(comps):
                lift_f[pl.ds(slot_lanes * t + comps * cz + c, 1), :] = spread[
                    c, pl.ds(3 * t + cz, 1), :
                ]
    base = lift_f[pl.ds(0, depth), :]
    low_half = lax.broadcasted_iota(jnp.int32, (depth, LANES), 1) < LANES // 2
    for k in range(TILE // 2):
        even = pltpu.roll(base, comps * 2 * k, 0) if k else base
        odd = pltpu.roll(base, comps * (2 * k + 1), 0)
        lift_w[:, LANES * k : LANES * (k + 1)] = jnp.where(low_half, even, odd).astype(BF16)

    rows_s, lanes_s = select_w.shape
    zw = size_z + 2 * TILE
    row = lax.broadcasted_iota(jnp.int32, (rows_s, LANES), 0)
    lane = lax.broadcasted_iota(jnp.int32, (rows_s, LANES), 1)
    place, inside = lax.div(lane, slot_lanes), lax.rem(lane, slot_lanes)
    level = lax.div(inside, comps)
    comp = inside - comps * level
    for k in range(quarters):
        source = lax.rem(place + quarters - k, quarters)
        target = comp * zw + TILE * source - 2 + level
        hit = (row == target) & (inside < comps * (TILE + 2))
        select_w[:, LANES * k : LANES * (k + 1)] = jnp.where(hit, 1.0, 0.0).astype(BF16)

    loads[2].wait()
    build_fine(encode_raw, encode_w, 0, encode_raw.shape[2], True)
    loads[4].wait()
    build_coarse(first_raw, first_w)
    loads[5].wait()
    build_coarse(second_raw, second_w)
    loads[7].wait()
    channels = decode_raw.shape[2] // 2
    build_fine(decode_raw, skip_w, 0, channels)
    build_fine(decode_raw, wide_w, channels, 2 * channels)
    loads[8].wait()
    head_f[...] = jnp.zeros(head_f.shape, F32)
    for p in range(2):
        for q in range(2):
            for c in range(comps):
                value = head_raw[pl.ds(c, 1), :].astype(F32)
                other = jnp.zeros_like(value)
                head_f[
                    pl.ds(LANES * p + size_z * c + q, 1), LANES * p : LANES * (p + 1)
                ] = jnp.concatenate([other, value] if q else [value, other], axis=1)
    head_w[...] = head_f[...].astype(BF16)
    unit[...] = jnp.ones(unit.shape, F32)
    loads[3].wait()
    loads[6].wait()

    for copy in copies:
        copy.wait_recv()

    slots = window.shape[0]
    turned = jnp.concatenate(
        [
            jnp.swapaxes(window[s, r].astype(F32).reshape(comps * zw, LANES), 0, 1)
            for s in range(slots) for r in range(2)
        ],
        axis=0,
    ).astype(BF16)
    grouped = lax.dot_general(turned, select_w[...], NN, preferred_element_type=F32)
    tiles_y = size_y // TILE
    for s in range(slots):
        for r in range(2):
            part = grouped[LANES * (2 * s + r) : LANES * (2 * s + r + 1)]
            for k in range(quarters):
                joint[k, pl.ds(size_x * s, size_x), pl.ds(tiles_y * r, tiles_y)] = part[
                    :, LANES * k : LANES * (k + 1)
                ].reshape(size_x, tiles_y, TILE, LANES)
    planes_d, rows_n = near.shape[1], near.shape[2]
    first_tile = tiles_y - 2 - (tiles_y // 2) * mine_x
    for k in range(quarters):
        for x in range(planes_d):
            near[k, x] = joint[k, x, pl.ds(first_tile, rows_n // TILE)].reshape(rows_n, LANES)

    planes_f = fine_in.shape[2]
    planes_c, planes_m, planes_e = coarse_in.shape[1], middle_in.shape[1], deep_scr.shape[0]
    planes_u = wide_in.shape[1]

    def source(plane, tap, total, shift=0):
        if around:
            if isinstance(plane, int):
                return (plane + tap - 1) % total
            return lax.rem(plane + tap + total - 1, total)
        return plane + tap + shift

    half_y = rows_n // 3
    slot_of = lax.div(lax.broadcasted_iota(jnp.int32, (half_y, LANES), 1), slot_lanes)

    @pl.loop(0, planes_f)
    def _(x):
        for parity in range(2):
            for q in range(quarters):
                for g in range(3):
                    taps = list(range(quarters * g, min(quarters * (g + 1), 9)))
                    value = None
                    for j, t in enumerate(taps):
                        part = near[
                            (j - q) % quarters, source(x, t // 3, planes_d),
                            pl.ds(TILE - 1 + parity + t % 3, half_y, stride=2), :,
                        ]
                        value = part if value is None else jnp.where(slot_of < j, value, part)
                    lift_rows[
                        q, pl.ds(pl.multiple_of(2 * half_y * x + half_y * parity, half_y), half_y),
                        LANES * g : LANES * (g + 1),
                    ] = value.astype(BF16)

    zpairs = zw // 2
    def lifted(q):
        return leaky(
            lax.dot_general(lift_rows[q], lift_w[...], NN, preferred_element_type=F32)
        )

    following = lifted(0)
    for q in range(quarters):
        value = following
        following = lifted(q + 1) if q + 1 < quarters else None
        for r in range(quarters):
            zp = quarters * q + r
            for x in range(planes_f):
                even, odd = (
                    value[
                        half_y * (2 * x + parity) : half_y * (2 * x + parity + 1),
                        LANES * r : LANES * (r + 1),
                    ]
                    for parity in range(2)
                )
                for b, part in enumerate(
                    (pltpu.roll(odd, 1, 0), even, odd, pltpu.roll(even, half_y - 1, 0))
                ):
                    fine_in[b, zp, x] = part.astype(BF16)

    inner = zpairs - 2
    quarter = TILE // 2
    own = zpairs - TILE
    low = lax.broadcasted_iota(jnp.int32, (own * TILE, LANES), 1) < LANES // 2

    def store_pairs(target, x, levels):
        for b in range(4):
            shift = quarter + (-1, 0, 0, 1)[b]
            start = LANES * ((b + 1) % 2)
            parts = [
                pltpu.roll(level[:, start : start + LANES], half_y - shift, 0)[:TILE]
                for level in levels
            ]
            plane, above, below = (
                jnp.concatenate(parts[d : d + own], axis=0) for d in (1, 2, 0)
            )
            target[b, x] = jnp.concatenate(
                [plane, jnp.where(low, above, below)], axis=1
            ).astype(BF16)

    def store_coarse(target, x, z, value):
        lanes = slice(LANES * (z % 2), LANES * (z % 2) + LANES)
        for b, part in enumerate((pltpu.roll(value, 1, 0), value, pltpu.roll(value, half_y - 1, 0))):
            target[b, x, z // 2, :, lanes] = part.astype(BF16)

    rows_e = inner * half_y

    def joined(sums):
        return sums[0] + sums[1] * unit[...]

    def encode(x):
        skip_scr = skip_two.at[x % 2]
        sums = [None, None]
        for a in range(3):
            for b in range(4):
                lhs = jnp.concatenate(
                    [
                        jnp.concatenate(
                            [
                                fine_in[
                                    b, pl.ds(d, inner), source(2 * x + g, a, planes_f)
                                ].reshape(rows_e, LANES)
                                for d in (1, 2)
                            ],
                            axis=1,
                        )
                        for g in range(2)
                    ],
                    axis=0,
                )
                term = dot(lhs, encode_w[4 * a + b])
                sums[b % 2] = term if sums[b % 2] is None else sums[b % 2] + term
        skip_scr[...] = rounded(joined(sums))

    def encoded(x):
        skip_scr = skip_two.at[x % 2]
        coarse = None
        for g in range(2):
            part = skip_scr[g * rows_e : (g + 1) * rows_e]
            term = lax.dot_general(part, downward_w[g], NN, preferred_element_type=F32)
            coarse = term if coarse is None else coarse + term
        coarse = rounded(coarse).astype(F32)
        for z in range(inner):
            store_coarse(coarse_in, x, z, coarse[half_y * z : half_y * (z + 1)])

    def kept(x):
        skip_scr = skip_two.at[x % 2]
        skirt = (inner - own) // 2 - 1
        for g in range(2):
            levels = [
                skip_scr[pl.ds(g * rows_e + half_y * (skirt + z), half_y)].astype(F32)
                for z in range(own + 2)
            ]
            store_pairs(skip_in, 2 * x + g, levels)

    encode(0)

    for x in range(1, planes_c):
        encode(x)
        encoded(x - 1)
        kept(x - 1)

    encoded(planes_c - 1)

    def coarse_conv(target, weight, planes, count):
        total = target.shape[1]
        sums = [None, None]
        for a in range(3):
            for b in range(3):
                for offset in range(2):
                    lhs = jnp.concatenate(
                        [
                            target[
                                b, (x + a - 1) % total if around else x + a,
                                offset : offset + count,
                            ].reshape(count * half_y, 2 * LANES)
                            for x in range(planes)
                        ],
                        axis=0,
                    )
                    term = dot(lhs, weight[6 * a + 2 * b + offset])
                    sums[offset] = term if sums[offset] is None else sums[offset] + term
        return joined(sums)

    def decode(array, weight, side, shift, taps):
        sums = [None, None]
        for number, (a, b) in enumerate(taps):
            lhs = jnp.concatenate(
                [
                    array[b, source(size_x * side + g, a, array.shape[1], shift)]
                    for g in range(size_x)
                ],
                axis=0,
            )
            term = dot(lhs, weight[4 * a + b])
            n = number % 2
            sums[n] = term if sums[n] is None else sums[n] + term
        return joined(sums)

    taps = [(a, b) for a in range(3) for b in range(4)]
    count = inner // 2 - 1
    middle = coarse_conv(coarse_in, first_w, planes_m, count)
    kept(planes_c - 1)
    ahead[...] = decode(skip_in, skip_w, 1 - mine_x, 5, taps[:6])
    middle = rounded(middle).astype(F32)
    for x in range(planes_m):
        for z in range(2 * count):
            start = half_y * (count * x + z // 2)
            store_coarse(
                middle_in, x, z,
                middle[start : start + half_y, LANES * (z % 2) : LANES * (z % 2) + LANES],
            )
    count -= 1
    deep = coarse_conv(middle_in, second_w, planes_e, count)
    ahead[...] += decode(skip_in, skip_w, 1 - mine_x, 5, taps[6:])
    deep_scr[...] = rounded(deep).reshape(planes_e, count * half_y, 2 * LANES)

    for x in range(planes_e):
        sides = [deep_scr[x, :, LANES * side : LANES * (side + 1)] for side in range(2)]
        for a in range(2):
            values = [rounded(dot(lhs, up_w[a])).astype(F32) for lhs in sides]
            levels = [
                values[z % 2][half_y * (z // 2) : half_y * (z // 2 + 1)] for z in range(own + 2)
            ]
            store_pairs(wide_in, 2 * x + a, levels)

    swap = None
    for turn in range(2):
        side = mine_x if turn else 1 - mine_x
        if turn:
            ahead[...] = decode(skip_in, skip_w, side, 5, taps)
        summed = ahead[...] + decode(wide_in, wide_w, side, 1, taps)
        result = dot(rounded(summed), head_w[...])
        for p in range(2):
            totals = []
            for g in range(size_x):
                total = None
                for z in range(own):
                    start = TILE * (own * g + z)
                    value = result[start : start + TILE, LANES * p : LANES * (p + 1)]
                    value = pltpu.roll(value, 2 * z, 1) if z else value
                    total = value if total is None else total + value
                totals.append(total)
            for g in range(size_x // 2):
                total = totals[g] + pltpu.roll(totals[g + size_x // 2], LANES // 2, 1)
                if turn:
                    final[g, mine_x, pl.ds(p, TILE, stride=2), :] = total
                else:
                    mine[g, pl.ds(p, TILE, stride=2), :] = total
        if not turn:
            swap = pltpu.make_async_remote_copy(
                src_ref=mine, dst_ref=final.at[:, mine_x],
                send_sem=swap_sems.at[0], recv_sem=swap_sems.at[1],
                device_id=device(0, 1, 0, 0), device_id_type=MESH,
            )
            swap.start()
    swap.wait_recv()
    flat = jnp.swapaxes(final[...].reshape(LANES // 2, LANES), 0, 1)
    for c in range(comps):
        for x in range(size_x):
            start = LANES // 2 * (2 * x // size_x) + size_z * c
            shift = size_y * (x % (size_x // 2))
            out_ref[c, x] = cells[c, x].astype(F32) + flat[
                start : start + size_z, shift : shift + size_y
            ]
    for copy in copies:
        copy.wait_send()
    swap.wait_send()


def local(
    rings, displacement, lift_weight, encode_weight, downward_weight, middle_first, middle_second,
    up_weight, decode_weight, head_weight,
):
    comps, size_x, size_y, size_z = displacement.shape
    c1, c2 = encode_weight.shape[1], middle_first.shape[1]
    around = rings[0] == 2
    slots = 2 if around else 6
    span = 2 * size_x
    halo = (lambda h: 0) if around else (lambda h: h)
    zw, yh = size_z + 2 * TILE, (size_y // 2 + 2 * TILE) // 2
    zpairs, quarters = zw // 2, zw // TILE
    planes_d, planes_f, planes_s = (span + 2 * halo(h) for h in (8, 7, 6))
    planes_c, planes_m, planes_e = (span // 2 + 2 * halo(h) for h in (3, 2, 1))
    depth = 3 * LANES

    cells = jnp.transpose(displacement, (0, 1, 3, 2))
    lift = jnp.transpose(lift_weight, (2, 0, 1))
    downward = jnp.transpose(downward_weight, (0, 2, 1)).reshape(2, 4 * c1, c2)
    up_w = up_weight.reshape(2, 4 * c1, c2)
    anywhere = pl.BlockSpec(memory_space=pltpu.HBM)
    links = (11 if around else 35)
    v = pltpu.VMEM
    result = pl.pallas_call(
        functools.partial(unet, rings),
        out_shape=pltpu.VMEM(cells.shape, F32),
        in_specs=[anywhere] * 9,
        out_specs=pl.BlockSpec(memory_space=pltpu.VMEM),
        scratch_shapes=[
            v(cells.shape, BF16), v(lift.shape, BF16), v(head_weight.shape, BF16),
            v((comps, size_z // TILE, TILE, LANES), BF16),
            v((slots, 2, comps, quarters, TILE, LANES), BF16),
            v((quarters, size_x * slots, 2 * size_y // TILE, TILE, LANES), F32),
            v((quarters, planes_d, 3 * yh, LANES), F32),
            v((comps, lift.shape[1], LANES), F32), v((depth, LANES), F32),
            v((quarters, planes_f * 2 * yh, depth), BF16),
            v((depth, quarters * LANES), BF16),
            v((comps * zw, quarters * LANES), BF16),
            v((4, zpairs, planes_f, yh, LANES), BF16),
            v((2, 2 * (zpairs - 2) * yh, 2 * LANES), BF16),
            v((4, planes_s, (zpairs - TILE) * TILE, 2 * LANES), BF16),
            v((4, 2 * planes_e, (zpairs - TILE) * TILE, 2 * LANES), BF16),
            v((3, planes_c, zpairs // 2 - 1, yh, 2 * LANES), BF16),
            v((3, planes_m, zpairs // 2 - 2, yh, 2 * LANES), BF16),
            v((planes_e, (zpairs // 2 - 3) * yh, 2 * LANES), BF16),
            v((size_x // 2, 2 * TILE, LANES), F32),
            v((size_x // 2, 2, 2 * TILE, LANES), F32),
            v((size_x * (zpairs - TILE) * TILE, 2 * LANES), F32),
            v((2 * LANES, 2 * LANES), F32), v((2 * LANES, 2 * LANES), BF16), v((1, 2 * LANES), F32),
            v(encode_weight.shape, BF16), v(downward.shape, BF16), v(middle_first.shape, BF16),
            v(middle_second.shape, BF16), v(up_w.shape, BF16), v(decode_weight.shape, BF16),
            v((12, 4 * c1, 4 * c1), BF16), v((12, 4 * c1, 4 * c1), BF16),
            v((12, 4 * c1, 4 * c1), BF16),
            v((18, 2 * c2, 2 * c2), BF16), v((18, 2 * c2, 2 * c2), BF16),
            pltpu.SemaphoreType.DMA((9,)),
            pltpu.SemaphoreType.DMA((links,)), pltpu.SemaphoreType.DMA((links,)),
            pltpu.SemaphoreType.DMA((2,)),
        ],
        compiler_params=pltpu.CompilerParams(
            collective_id=0, has_side_effects=True, vmem_limit_bytes=63 * 2**20
        ),
    )(
        cells, lift, encode_weight, downward, middle_first, middle_second, up_w, decode_weight,
        head_weight,
    )
    return jnp.transpose(result, (0, 1, 3, 2))


def solution(mesh):
    placed = (P(None, "gx", "gy", "gz"), P(), P(), P(), P(), P(), P(), P(), P())
    rings = tuple(mesh.shape[axis] for axis in ("gx", "gy", "gz"))
    return jax.shard_map(
        functools.partial(local, rings), mesh=mesh, in_specs=placed,
        out_specs=P(None, "gx", "gy", "gz"), check_vma=False,
    )
```

```python
import functools

import jax
import jax.numpy as jnp
from jax import lax
from jax.experimental import pallas as pl
from jax.experimental.pallas import tpu as pltpu
from jax.sharding import PartitionSpec as P

MESH = pl.DeviceIdType.MESH
NT = (((1,), (1,)), ((), ()))
NN = (((1,), (0,)), ((), ()))
F32, BF16 = jnp.float32, jnp.bfloat16
TILE, LANES = 8, 128


def leaky(value):
    return jnp.maximum(value, 0.1 * value)


def rounded(value):
    return leaky(value).astype(BF16)


def dot(rows, weight):
    return lax.dot_general(rows, weight, NT, preferred_element_type=F32)


def build_fine(raw, wide, lo, hi, odd=False):
    out = raw.shape[1]
    blank = jnp.zeros((2 * out, wide.shape[2]), BF16)
    zero = jnp.zeros((out, hi - lo), BF16)
    for a in range(3):
        wide[4 * a, 2 * out :, :] = blank
        wide[4 * a + 3, : 2 * out, :] = blank
        for b in range(3):
            taps = [raw[9 * a + 3 * b + c][:, lo:hi] for c in range(3)]
            if odd:
                low = jnp.concatenate([taps[0], taps[1], taps[2], zero], axis=1)
                high = jnp.concatenate([zero, taps[0], taps[1], taps[2]], axis=1)
            else:
                low = jnp.concatenate([taps[1], taps[2], zero, taps[0]], axis=1)
                high = jnp.concatenate([taps[0], taps[1], taps[2], zero], axis=1)
            pair = jnp.concatenate([low, high], axis=0)
            wide[4 * a + b, : 2 * out, :] = pair
            wide[4 * a + b + 1, 2 * out :, :] = pair


def build_coarse(raw, wide):
    out = raw.shape[1]
    blank = jnp.zeros((out, raw.shape[2]), BF16)
    for a in range(3):
        for b in range(3):
            for offset in range(2):
                tile = 6 * a + 2 * b + offset
                for side in range(2):
                    for e in range(2):
                        c = 2 * offset + e - side
                        block = raw[9 * a + 3 * b + c] if 0 <= c <= 2 else blank
                        wide[tile, out * side : out * (side + 1), LANES * e : LANES * (e + 1)] = block


def unet(
    dims,
    cells_hbm, lift_hbm, encode_hbm, downward_hbm, first_hbm, second_hbm, up_hbm, decode_hbm,
    head_hbm,
    out_ref,
    cells, lift_raw, head_raw, pack, window, joint, near, spread, lift_f, lift_rows, lift_w, select_w,
    fine_in, skip_two, skip_in, wide_in, coarse_in, middle_in, deep_scr, mine, final, ahead,
    head_f, head_w, unit,
    encode_raw, downward_w, first_raw, second_raw, up_w, decode_raw,
    encode_w, skip_w, wide_w, first_w, second_w,
    load_sems, send_sems, recv_sems, swap_sems,
):
    ring_x, ring_y, ring_z = dims
    comps, size_x, size_z, size_y = cells.shape
    around = ring_x == 2
    steps = (0,) if around else (-1, 0, 1)
    pairs = ring_x // 2
    gx, gy, gz = lax.axis_index("gx"), lax.axis_index("gy"), lax.axis_index("gz")
    mine_x, pair = lax.rem(gx, 2), lax.div(gx, 2)

    def device(step, flip, shift_y, shift_z):
        side = 1 - mine_x if flip else mine_x
        return (
            2 * lax.rem(pair + pairs + step, pairs) + side,
            lax.rem(gy + ring_y + shift_y, ring_y),
            lax.rem(gz + ring_z + shift_z, ring_z),
        )

    links = [
        (step, flip, beside, dz)
        for step in steps for flip in (0, 1) for beside in (0, 1) for dz in (-1, 0, 1)
        if (step, flip, beside, dz) != (0, 0, 0, 0)
    ]
    barrier = pltpu.get_barrier_semaphore()
    for step, flip, beside, dz in links:
        shift = 2 * mine_x - 1 if beside else 0
        pl.semaphore_signal(
            barrier, inc=1, device_id=device(step, flip, shift, -dz), device_id_type=MESH
        )
    loads = [
        pltpu.make_async_copy(src, dst, load_sems.at[i])
        for i, (src, dst) in enumerate(
            (
                (cells_hbm, cells), (lift_hbm, lift_raw), (encode_hbm, encode_raw),
                (downward_hbm, downward_w), (first_hbm, first_raw), (second_hbm, second_raw),
                (up_hbm, up_w), (decode_hbm, decode_raw), (head_hbm, head_raw),
            )
        )
    ]
    for load in loads:
        load.start()

    loads[0].wait()
    for c in range(comps):
        total = None
        for x in range(size_x):
            value = cells[c, x].astype(F32)
            value = jnp.concatenate(
                [value, jnp.zeros((size_z, LANES - size_y), F32)], axis=1
            )
            value = pltpu.roll(value, size_y * x, 1) if x else value
            total = value if total is None else total + value
        pack[c] = total.reshape(size_z // TILE, TILE, LANES).astype(BF16)
    own_slot = mine_x if around else mine_x + 2
    tiles = size_z // TILE
    window[own_slot, 1 - mine_x, :, pl.ds(1, tiles)] = pack[...]
    pl.semaphore_wait(barrier, len(links))
    copies = []
    for number, (step, flip, beside, dz) in enumerate(links):
        side = 1 - mine_x if flip else mine_x
        shift = 1 - 2 * side if beside else 0
        row_slot = side if beside else 1 - side
        slot = mine_x if around else mine_x + 2 * (step + 1)
        start, count, place = {0: (0, tiles, 1), 1: (tiles - 1, 1, 0), -1: (0, 1, tiles + 1)}[dz]
        copies.append(
            pltpu.make_async_remote_copy(
                src_ref=pack.at[:, pl.ds(start, count)],
                dst_ref=window.at[slot, row_slot, :, pl.ds(place, count)],
                send_sem=send_sems.at[number], recv_sem=recv_sems.at[number],
                device_id=device(-step, flip, shift, dz), device_id_type=MESH,
            )
        )
    for copy in copies:
        copy.start()

    loads[1].wait()
    quarters = (size_z + 2 * TILE) // TILE
    slot_lanes = LANES // quarters
    for c in range(comps):
        value = lift_raw[c].astype(F32)
        spread[c] = jnp.concatenate([value, value], axis=1)
    depth = lift_w.shape[0]
    lift_f[pl.ds(0, depth), :] = jnp.zeros((depth, LANES), F32)
    for t in range(9):
        for cz in range(3):
            for c in range(comps):
                lift_f[pl.ds(slot_lanes * t + comps * cz + c, 1), :] = spread[
                    c, pl.ds(3 * t + cz, 1), :
                ]
    base = lift_f[pl.ds(0, depth), :]
    low_half = lax.broadcasted_iota(jnp.int32, (depth, LANES), 1) < LANES // 2
    for k in range(TILE // 2):
        even = pltpu.roll(base, comps * 2 * k, 0) if k else base
        odd = pltpu.roll(base, comps * (2 * k + 1), 0)
        lift_w[:, LANES * k : LANES * (k + 1)] = jnp.where(low_half, even, odd).astype(BF16)

    rows_s, lanes_s = select_w.shape
    zw = size_z + 2 * TILE
    row = lax.broadcasted_iota(jnp.int32, (rows_s, LANES), 0)
    lane = lax.broadcasted_iota(jnp.int32, (rows_s, LANES), 1)
    place, inside = lax.div(lane, slot_lanes), lax.rem(lane, slot_lanes)
    level = lax.div(inside, comps)
    comp = inside - comps * level
    for k in range(quarters):
        source = lax.rem(place + quarters - k, quarters)
        target = comp * zw + TILE * source - 2 + level
        hit = (row == target) & (inside < comps * (TILE + 2))
        select_w[:, LANES * k : LANES * (k + 1)] = jnp.where(hit, 1.0, 0.0).astype(BF16)

    loads[2].wait()
    build_fine(encode_raw, encode_w, 0, encode_raw.shape[2], True)
    loads[4].wait()
    build_coarse(first_raw, first_w)
    loads[5].wait()
    build_coarse(second_raw, second_w)
    loads[7].wait()
    channels = decode_raw.shape[2] // 2
    build_fine(decode_raw, skip_w, 0, channels)
    build_fine(decode_raw, wide_w, channels, 2 * channels)
    loads[8].wait()
    head_f[...] = jnp.zeros(head_f.shape, F32)
    for p in range(2):
        for q in range(2):
            for c in range(comps):
                value = head_raw[pl.ds(c, 1), :].astype(F32)
                other = jnp.zeros_like(value)
                head_f[
                    pl.ds(LANES * p + size_z * c + q, 1), LANES * p : LANES * (p + 1)
                ] = jnp.concatenate([other, value] if q else [value, other], axis=1)
    head_w[...] = head_f[...].astype(BF16)
    unit[...] = jnp.ones(unit.shape, F32)
    loads[3].wait()
    loads[6].wait()

    for copy in copies:
        copy.wait_recv()

    slots = window.shape[0]
    turned = jnp.concatenate(
        [
            jnp.swapaxes(window[s, r].astype(F32).reshape(comps * zw, LANES), 0, 1)
            for s in range(slots) for r in range(2)
        ],
        axis=0,
    ).astype(BF16)
    grouped = lax.dot_general(turned, select_w[...], NN, preferred_element_type=F32)
    tiles_y = size_y // TILE
    for s in range(slots):
        for r in range(2):
            part = grouped[LANES * (2 * s + r) : LANES * (2 * s + r + 1)]
            for k in range(quarters):
                joint[k, pl.ds(size_x * s, size_x), pl.ds(tiles_y * r, tiles_y)] = part[
                    :, LANES * k : LANES * (k + 1)
                ].reshape(size_x, tiles_y, TILE, LANES)
    planes_d, rows_n = near.shape[1], near.shape[2]
    first_tile = tiles_y - 2 - (tiles_y // 2) * mine_x
    for k in range(quarters):
        for x in range(planes_d):
            near[k, x] = joint[k, x, pl.ds(first_tile, rows_n // TILE)].reshape(rows_n, LANES)

    planes_f = fine_in.shape[2]
    planes_c, planes_m, planes_e = coarse_in.shape[1], middle_in.shape[1], deep_scr.shape[0]
    planes_u = wide_in.shape[1]

    def source(plane, tap, total, shift=0):
        if around:
            if isinstance(plane, int):
                return (plane + tap - 1) % total
            return lax.rem(plane + tap + total - 1, total)
        return plane + tap + shift

    half_y = rows_n // 3
    slot_of = lax.div(lax.broadcasted_iota(jnp.int32, (half_y, LANES), 1), slot_lanes)

    def rows_of(q):
        for x in range(planes_f):
            for parity in range(2):
                for g in range(3):
                    taps = list(range(quarters * g, min(quarters * (g + 1), 9)))
                    value = None
                    for j, t in enumerate(taps):
                        part = near[
                            (j - q) % quarters, source(x, t // 3, planes_d),
                            pl.ds(TILE - 1 + parity + t % 3, half_y, stride=2), :,
                        ]
                        value = part if value is None else jnp.where(slot_of < j, value, part)
                    lift_rows[
                        q, pl.ds(half_y * (2 * x + parity), half_y),
                        LANES * g : LANES * (g + 1),
                    ] = value.astype(BF16)

    zpairs = zw // 2
    def lifted(q):
        rows_of(q)
        return leaky(
            lax.dot_general(lift_rows[q], lift_w[...], NN, preferred_element_type=F32)
        )

    following = lifted(0)
    for q in range(quarters):
        value = following
        following = lifted(q + 1) if q + 1 < quarters else None
        for r in range(quarters):
            zp = quarters * q + r
            for x in range(planes_f):
                even, odd = (
                    value[
                        half_y * (2 * x + parity) : half_y * (2 * x + parity + 1),
                        LANES * r : LANES * (r + 1),
                    ]
                    for parity in range(2)
                )
                for b, part in enumerate(
                    (pltpu.roll(odd, 1, 0), even, odd, pltpu.roll(even, half_y - 1, 0))
                ):
                    fine_in[b, zp, x] = part.astype(BF16)

    inner = zpairs - 2
    quarter = TILE // 2
    own = zpairs - TILE
    low = lax.broadcasted_iota(jnp.int32, (own * TILE, LANES), 1) < LANES // 2

    def store_pairs(target, x, levels):
        for b in range(4):
            shift = quarter + (-1, 0, 0, 1)[b]
            start = LANES * ((b + 1) % 2)
            parts = [
                pltpu.roll(level[:, start : start + LANES], half_y - shift, 0)[:TILE]
                for level in levels
            ]
            plane, above, below = (
                jnp.concatenate(parts[d : d + own], axis=0) for d in (1, 2, 0)
            )
            target[b, x] = jnp.concatenate(
                [plane, jnp.where(low, above, below)], axis=1
            ).astype(BF16)

    def store_coarse(target, x, z, value):
        lanes = slice(LANES * (z % 2), LANES * (z % 2) + LANES)
        for b, part in enumerate((pltpu.roll(value, 1, 0), value, pltpu.roll(value, half_y - 1, 0))):
            target[b, x, z // 2, :, lanes] = part.astype(BF16)

    rows_e = inner * half_y

    def joined(sums):
        return sums[0] + sums[1] * unit[...]

    def encode(x):
        skip_scr = skip_two.at[x % 2]
        sums = [None, None]
        for a in range(3):
            for b in range(4):
                lhs = jnp.concatenate(
                    [
                        jnp.concatenate(
                            [
                                fine_in[
                                    b, pl.ds(d, inner), source(2 * x + g, a, planes_f)
                                ].reshape(rows_e, LANES)
                                for d in (1, 2)
                            ],
                            axis=1,
                        )
                        for g in range(2)
                    ],
                    axis=0,
                )
                term = dot(lhs, encode_w[4 * a + b])
                sums[b % 2] = term if sums[b % 2] is None else sums[b % 2] + term
        skip_scr[...] = rounded(joined(sums))

    def encoded(x):
        skip_scr = skip_two.at[x % 2]
        coarse = None
        for g in range(2):
            part = skip_scr[g * rows_e : (g + 1) * rows_e]
            term = lax.dot_general(part, downward_w[g], NN, preferred_element_type=F32)
            coarse = term if coarse is None else coarse + term
        coarse = rounded(coarse).astype(F32)
        for z in range(inner):
            store_coarse(coarse_in, x, z, coarse[half_y * z : half_y * (z + 1)])

    def kept(x):
        skip_scr = skip_two.at[x % 2]
        skirt = (inner - own) // 2 - 1
        for g in range(2):
            levels = [
                skip_scr[pl.ds(g * rows_e + half_y * (skirt + z), half_y)].astype(F32)
                for z in range(own + 2)
            ]
            store_pairs(skip_in, 2 * x + g, levels)

    encode(0)

    for x in range(1, planes_c):
        encode(x)
        encoded(x - 1)
        kept(x - 1)

    encoded(planes_c - 1)

    def coarse_conv(target, weight, planes, count):
        total = target.shape[1]
        sums = [None, None]
        for a in range(3):
            for b in range(3):
                for offset in range(2):
                    lhs = jnp.concatenate(
                        [
                            target[
                                b, (x + a - 1) % total if around else x + a,
                                offset : offset + count,
                            ].reshape(count * half_y, 2 * LANES)
                            for x in range(planes)
                        ],
                        axis=0,
                    )
                    term = dot(lhs, weight[6 * a + 2 * b + offset])
                    sums[offset] = term if sums[offset] is None else sums[offset] + term
        return joined(sums)

    def decode(array, weight, side, shift, taps):
        sums = [None, None]
        for number, (a, b) in enumerate(taps):
            lhs = jnp.concatenate(
                [
                    array[b, source(size_x * side + g, a, array.shape[1], shift)]
                    for g in range(size_x)
                ],
                axis=0,
            )
            term = dot(lhs, weight[4 * a + b])
            n = number % 2
            sums[n] = term if sums[n] is None else sums[n] + term
        return joined(sums)

    taps = [(a, b) for a in range(3) for b in range(4)]
    count = inner // 2 - 1
    middle = coarse_conv(coarse_in, first_w, planes_m, count)
    kept(planes_c - 1)
    ahead[...] = decode(skip_in, skip_w, 1 - mine_x, 5, taps[:6])
    middle = rounded(middle).astype(F32)
    for x in range(planes_m):
        for z in range(2 * count):
            start = half_y * (count * x + z // 2)
            store_coarse(
                middle_in, x, z,
                middle[start : start + half_y, LANES * (z % 2) : LANES * (z % 2) + LANES],
            )
    count -= 1
    deep = coarse_conv(middle_in, second_w, planes_e, count)
    ahead[...] += decode(skip_in, skip_w, 1 - mine_x, 5, taps[6:])
    deep_scr[...] = rounded(deep).reshape(planes_e, count * half_y, 2 * LANES)

    for x in range(planes_e):
        sides = [deep_scr[x, :, LANES * side : LANES * (side + 1)] for side in range(2)]
        for a in range(2):
            values = [rounded(dot(lhs, up_w[a])).astype(F32) for lhs in sides]
            levels = [
                values[z % 2][half_y * (z // 2) : half_y * (z // 2 + 1)] for z in range(own + 2)
            ]
            store_pairs(wide_in, 2 * x + a, levels)

    swap = None
    for turn in range(2):
        side = mine_x if turn else 1 - mine_x
        if turn:
            ahead[...] = decode(skip_in, skip_w, side, 5, taps)
        summed = ahead[...] + decode(wide_in, wide_w, side, 1, taps)
        result = dot(rounded(summed), head_w[...])
        for p in range(2):
            totals = []
            for g in range(size_x):
                total = None
                for z in range(own):
                    start = TILE * (own * g + z)
                    value = result[start : start + TILE, LANES * p : LANES * (p + 1)]
                    value = pltpu.roll(value, 2 * z, 1) if z else value
                    total = value if total is None else total + value
                totals.append(total)
            for g in range(size_x // 2):
                total = totals[g] + pltpu.roll(totals[g + size_x // 2], LANES // 2, 1)
                if turn:
                    final[g, mine_x, pl.ds(p, TILE, stride=2), :] = total
                else:
                    mine[g, pl.ds(p, TILE, stride=2), :] = total
        if not turn:
            swap = pltpu.make_async_remote_copy(
                src_ref=mine, dst_ref=final.at[:, mine_x],
                send_sem=swap_sems.at[0], recv_sem=swap_sems.at[1],
                device_id=device(0, 1, 0, 0), device_id_type=MESH,
            )
            swap.start()
    swap.wait_recv()
    flat = jnp.swapaxes(final[...].reshape(LANES // 2, LANES), 0, 1)
    for c in range(comps):
        for x in range(size_x):
            start = LANES // 2 * (2 * x // size_x) + size_z * c
            shift = size_y * (x % (size_x // 2))
            out_ref[c, x] = cells[c, x].astype(F32) + flat[
                start : start + size_z, shift : shift + size_y
            ]
    for copy in copies:
        copy.wait_send()
    swap.wait_send()


def local(
    rings, displacement, lift_weight, encode_weight, downward_weight, middle_first, middle_second,
    up_weight, decode_weight, head_weight,
):
    comps, size_x, size_y, size_z = displacement.shape
    c1, c2 = encode_weight.shape[1], middle_first.shape[1]
    around = rings[0] == 2
    slots = 2 if around else 6
    span = 2 * size_x
    halo = (lambda h: 0) if around else (lambda h: h)
    zw, yh = size_z + 2 * TILE, (size_y // 2 + 2 * TILE) // 2
    zpairs, quarters = zw // 2, zw // TILE
    planes_d, planes_f, planes_s = (span + 2 * halo(h) for h in (8, 7, 6))
    planes_c, planes_m, planes_e = (span // 2 + 2 * halo(h) for h in (3, 2, 1))
    depth = 3 * LANES

    cells = jnp.transpose(displacement, (0, 1, 3, 2))
    lift = jnp.transpose(lift_weight, (2, 0, 1))
    downward = jnp.transpose(downward_weight, (0, 2, 1)).reshape(2, 4 * c1, c2)
    up_w = up_weight.reshape(2, 4 * c1, c2)
    anywhere = pl.BlockSpec(memory_space=pltpu.HBM)
    links = (11 if around else 35)
    v = pltpu.VMEM
    result = pl.pallas_call(
        functools.partial(unet, rings),
        out_shape=pltpu.VMEM(cells.shape, F32),
        in_specs=[anywhere] * 9,
        out_specs=pl.BlockSpec(memory_space=pltpu.VMEM),
        scratch_shapes=[
            v(cells.shape, BF16), v(lift.shape, BF16), v(head_weight.shape, BF16),
            v((comps, size_z // TILE, TILE, LANES), BF16),
            v((slots, 2, comps, quarters, TILE, LANES), BF16),
            v((quarters, size_x * slots, 2 * size_y // TILE, TILE, LANES), F32),
            v((quarters, planes_d, 3 * yh, LANES), F32),
            v((comps, lift.shape[1], LANES), F32), v((depth, LANES), F32),
            v((quarters, planes_f * 2 * yh, depth), BF16),
            v((depth, quarters * LANES), BF16),
            v((comps * zw, quarters * LANES), BF16),
            v((4, zpairs, planes_f, yh, LANES), BF16),
            v((2, 2 * (zpairs - 2) * yh, 2 * LANES), BF16),
            v((4, planes_s, (zpairs - TILE) * TILE, 2 * LANES), BF16),
            v((4, 2 * planes_e, (zpairs - TILE) * TILE, 2 * LANES), BF16),
            v((3, planes_c, zpairs // 2 - 1, yh, 2 * LANES), BF16),
            v((3, planes_m, zpairs // 2 - 2, yh, 2 * LANES), BF16),
            v((planes_e, (zpairs // 2 - 3) * yh, 2 * LANES), BF16),
            v((size_x // 2, 2 * TILE, LANES), F32),
            v((size_x // 2, 2, 2 * TILE, LANES), F32),
            v((size_x * (zpairs - TILE) * TILE, 2 * LANES), F32),
            v((2 * LANES, 2 * LANES), F32), v((2 * LANES, 2 * LANES), BF16), v((1, 2 * LANES), F32),
            v(encode_weight.shape, BF16), v(downward.shape, BF16), v(middle_first.shape, BF16),
            v(middle_second.shape, BF16), v(up_w.shape, BF16), v(decode_weight.shape, BF16),
            v((12, 4 * c1, 4 * c1), BF16), v((12, 4 * c1, 4 * c1), BF16),
            v((12, 4 * c1, 4 * c1), BF16),
            v((18, 2 * c2, 2 * c2), BF16), v((18, 2 * c2, 2 * c2), BF16),
            pltpu.SemaphoreType.DMA((9,)),
            pltpu.SemaphoreType.DMA((links,)), pltpu.SemaphoreType.DMA((links,)),
            pltpu.SemaphoreType.DMA((2,)),
        ],
        compiler_params=pltpu.CompilerParams(
            collective_id=0, has_side_effects=True, vmem_limit_bytes=63 * 2**20
        ),
    )(
        cells, lift, encode_weight, downward, middle_first, middle_second, up_w, decode_weight,
        head_weight,
    )
    return jnp.transpose(result, (0, 1, 3, 2))


def solution(mesh):
    placed = (P(None, "gx", "gy", "gz"), P(), P(), P(), P(), P(), P(), P(), P())
    rings = tuple(mesh.shape[axis] for axis in ("gx", "gy", "gz"))
    return jax.shard_map(
        functools.partial(local, rings), mesh=mesh, in_specs=placed,
        out_specs=P(None, "gx", "gy", "gz"), check_vma=False,
    )
```
